32 devices in a mesh: replica: 2 (over x), data: 4 (over z), table: 4 (over y, core).
Axes of the slice: x: 2, y: 2, z: 4, core: 2. Of those that a mesh axis runs over, the one named last changes fastest.
Arguments:
- tokens: bfloat16 [2048, 768], P(('replica', 'data', 'table')), parts along dimension 0
- grad_out: bfloat16 [2048, 768], P(('replica', 'data', 'table')), parts along dimension 0
- table_u: bfloat16 [131072, 768], P(('replica', 'table')), parts along dimension 0
- table_v: bfloat16 [131072, 768], P(('replica', 'table')), parts along dimension 0
- wanted_ids: int32 [32, 128], P(('replica', 'data', 'table')), parts along dimension 0
- pick_idx: int32 [2048, 4, 32], P(('replica', 'data', 'table')), parts along dimension 0
- gate_val: float32 [2048, 4, 32], P(('replica', 'data', 'table')), parts along dimension 0
Outputs:
- output 1: bfloat16 [2048, 768], P(('replica', 'data', 'table')), parts along dimension 0
- output 2: bfloat16 [2048, 768], P(('replica', 'data', 'table')), parts along dimension 0
- output 3: bfloat16 [131072, 768], P(('replica', 'table')), parts along dimension 0
- output 4: bfloat16 [131072, 768], P(('replica', 'table')), parts along dimension 0
There are 2 independent parts. The reference program is written for one: setup_inputs(seed, part) draws one part's arguments, and reference() takes and returns one part's arrays. A program takes and returns all parts, laid end to end along the dimension named above; each array names one.
All inputs are finite; a program needn't handle non-finite values.
Results may differ from the reference program's by a relative error of at most 0.00789345.
Values are sent between devices in bfloat16 or wider.
A program may use at most 1 GiB of HBM per device.

```python
import math
import jax
import jax.numpy as jnp
from jax import lax

D = 768
N = 65536
HEADS = 4
TOPK = 32
TOK_DEV = 64
DATA = 4
TABLE = 4
POOL = 32

N_LOCAL = N // TABLE
DEVS = DATA * TABLE
T_PART = DEVS * TOK_DEV
SEL_TOK = HEADS * TOPK
SEL_DEV = TOK_DEV * SEL_TOK
ENTRIES = TABLE * POOL
BLOCK = math.gcd(TOK_DEV, max(1, 8192 // SEL_TOK))


def draw_routing(route_key):
    perm_key, off_key, own_key_a, own_key_b, slot_key, mix_key = jax.random.split(route_key, 6)
    orders = jax.vmap(lambda one_key: jax.random.permutation(one_key, N_LOCAL))(jax.random.split(perm_key, TABLE))
    offsets = jax.random.randint(off_key, (DEVS, TABLE, 1), 0, 2 * POOL)
    spot_idx = (offsets + jnp.arange(POOL, dtype=jnp.int32)[None, None, :]) % N_LOCAL
    owner_idx = jnp.arange(TABLE, dtype=jnp.int32)[None, :, None]
    local_rows = orders[owner_idx, spot_idx]
    wanted = (local_rows + owner_idx * N_LOCAL).reshape(DEVS, ENTRIES).astype(jnp.int32)
    extra_len = SEL_DEV - ENTRIES
    own_a = jax.random.randint(own_key_a, (DEVS, extra_len), 0, TABLE)
    own_b = jax.random.randint(own_key_b, (DEVS, extra_len), 0, TABLE)
    slot_idx = jax.random.randint(slot_key, (DEVS, extra_len), 0, POOL)
    extra_picks = jnp.minimum(own_a, own_b) * POOL + slot_idx
    cover = jnp.broadcast_to(jnp.arange(ENTRIES, dtype=jnp.int32)[None, :], (DEVS, ENTRIES))
    pick_all = jnp.concatenate([cover, extra_picks.astype(jnp.int32)], axis=1)
    shuffle = jax.vmap(lambda one_key: jax.random.permutation(one_key, SEL_DEV))(jax.random.split(mix_key, DEVS))
    pick_all = jnp.take_along_axis(pick_all, shuffle, axis=1)
    return wanted, pick_all.reshape(T_PART, HEADS, TOPK).astype(jnp.int32)


def setup_inputs(seed: int = 0, part: int = 0) -> dict:
    part_key = jax.random.fold_in(jax.random.key(seed), part)
    key_list = jax.random.split(part_key, 6)
    tokens = jax.random.normal(key_list[0], (T_PART, D), jnp.float32).astype(jnp.bfloat16)
    grad_out = jax.random.normal(key_list[1], (T_PART, D), jnp.float32).astype(jnp.bfloat16)
    table_u = (jax.random.normal(key_list[2], (N, D), jnp.float32) * D ** -0.5).astype(jnp.bfloat16)
    table_v = (jax.random.normal(key_list[3], (N, D), jnp.float32) * SEL_TOK ** -0.5).astype(jnp.bfloat16)
    wanted_ids, pick_idx = draw_routing(key_list[4])
    gate_val = jax.random.uniform(key_list[5], (T_PART, HEADS, TOPK), jnp.float32, 0.5, 1.5)
    return {'tokens': tokens, 'grad_out': grad_out, 'table_u': table_u, 'table_v': table_v, 'wanted_ids': wanted_ids, 'pick_idx': pick_idx, 'gate_val': gate_val}


def gelu_pair(pre_act):
    cdf_val = 0.5 * (1.0 + lax.erf(pre_act * 0.7071067811865476))
    pdf_val = jnp.exp(-0.5 * pre_act * pre_act) * 0.3989422804014327
    return pre_act * cdf_val, cdf_val + pre_act * pdf_val


def reference(tokens, grad_out, table_u, table_v, wanted_ids, pick_idx, gate_val):
    sel_ids = jnp.take_along_axis(wanted_ids, pick_idx.reshape(DEVS, SEL_DEV), axis=1)
    num_blocks = T_PART // BLOCK
    inputs = (tokens.reshape(num_blocks, BLOCK, D), grad_out.reshape(num_blocks, BLOCK, D), sel_ids.reshape(num_blocks, BLOCK, SEL_TOK), gate_val.reshape(num_blocks, BLOCK, SEL_TOK))

    def body(acc_pair, block_in):
        acc_u, acc_v = acc_pair
        x_blk, dy_blk, id_blk, gate_blk = block_in
        x_f = x_blk.astype(jnp.float32)
        dy_f = dy_blk.astype(jnp.float32)
        sel_u = jnp.take(table_u, id_blk, axis=0).astype(jnp.float32)
        sel_v = jnp.take(table_v, id_blk, axis=0).astype(jnp.float32)
        pre_act = jnp.einsum('bsd,bd->bs', sel_u, x_f)
        act_val, slope_val = gelu_pair(pre_act)
        weight = gate_blk * act_val
        y_blk = jnp.einsum('bs,bsd->bd', weight, sel_v)
        v_dot_dy = jnp.einsum('bsd,bd->bs', sel_v, dy_f)
        coef_sel = gate_blk * slope_val * v_dot_dy
        dx_blk = jnp.einsum('bs,bsd->bd', coef_sel, sel_u)
        flat_ids = id_blk.reshape(-1)
        acc_u = acc_u.at[flat_ids].add((coef_sel[:, :, None] * x_f[:, None, :]).reshape(-1, D))
        acc_v = acc_v.at[flat_ids].add((weight[:, :, None] * dy_f[:, None, :]).reshape(-1, D))
        return (acc_u, acc_v), (y_blk.astype(jnp.bfloat16), dx_blk.astype(jnp.bfloat16))

    zero_acc = jnp.zeros((N, D), jnp.float32)
    (acc_u, acc_v), (y_st, dx_st) = lax.scan(body, (zero_acc, zero_acc), inputs)
    return (y_st.reshape(T_PART, D), dx_st.reshape(T_PART, D), acc_u.astype(jnp.bfloat16), acc_v.astype(jnp.bfloat16))
```

```python
import functools

import jax
import jax.numpy as jnp
from jax import lax
from jax.experimental import pallas as pl
from jax.experimental.pallas import tpu as pltpu
from jax.sharding import PartitionSpec as P

MESH = pl.DeviceIdType.MESH
F32 = jnp.float32
BF16 = jnp.bfloat16
VMEM = pl.BlockSpec(memory_space=pltpu.VMEM)
ANY = pl.BlockSpec(memory_space=pl.ANY)
NT = (((1,), (1,)), ((), ()))
TN = (((0,), (0,)), ((), ()))
BIG = 60 * 1024 * 1024


def gelu_pair(pre_act):
    cdf_val = 0.5 * (1.0 + lax.erf(pre_act * 0.7071067811865476))
    pdf_val = jnp.exp(-0.5 * pre_act * pre_act) * 0.3989422804014327
    return pre_act * cdf_val, cdf_val + pre_act * pdf_val


def split3(val):
    one = val.astype(BF16)
    rest = val - one.astype(F32)
    two = rest.astype(BF16)
    three = (rest - two.astype(F32)).astype(BF16)
    return one, two, three


def dot(a, b, dims=None):
    if dims is None:
        return jnp.dot(a, b, preferred_element_type=F32)
    return lax.dot_general(a, b, dims, preferred_element_type=F32)


def gate_kernel(pick_ref, gate_ref, ids_ref, out_ref):
    sel, tok = pick_ref.shape
    half = sel // 2
    row = lax.broadcasted_iota(jnp.int32, (half, 2 * tok), 0)

    def body(i, acc):
        base = pl.multiple_of(i * 8, 8)
        pick = pick_ref[pl.ds(base, 8), :]
        gate = gate_ref[pl.ds(base, 8), :]
        pick = jnp.concatenate([pick, pick - half], axis=1)
        gate = jnp.concatenate([gate, gate], axis=1)
        for j in range(8):
            acc = acc + jnp.where(row == pick[j : j + 1, :], gate[j : j + 1, :], 0.0)
        return acc

    out_ref[0:half, :] = lax.fori_loop(0, sel // 8, body, jnp.zeros((half, 2 * tok), F32))
    out_ref[half : half + 8, :] = jnp.broadcast_to(ids_ref[...].astype(F32), (8, sel))


def share_kernel(x_ref, dy_ref, g_ref, tx, ty, gx, ssem, rsem):
    z = lax.axis_index("data")
    t = lax.axis_index("table")
    last = 3
    y, c = t // 2, lax.rem(t, 2)
    y_peer = {"table": (1 - y) * 2 + c}
    c_peer = {"table": y * 2 + (1 - c)}
    up, down = {"data": z + 1}, {"data": z - 1}
    me = z * 4 + t
    tok = x_ref.shape[0]

    bar = pltpu.get_barrier_semaphore()
    for peer in (y_peer, c_peer):
        pl.semaphore_signal(bar, inc=1, device_id=peer, device_id_type=MESH)

    @pl.when(z < last)
    def _():
        pl.semaphore_signal(bar, inc=1, device_id=up, device_id_type=MESH)

    @pl.when(z > 0)
    def _():
        pl.semaphore_signal(bar, inc=1, device_id=down, device_id_type=MESH)

    pl.semaphore_wait(bar, 2 + (z < last).astype(jnp.int32) + (z > 0).astype(jnp.int32))

    own = (g_ref, x_ref, dy_ref)
    outs = (gx, tx, ty)

    def place(k, slot):
        if k == 0:
            return gx.at[slot]
        return outs[k].at[pl.ds(pl.multiple_of(slot * tok, tok), tok), :]

    def copy(k, slot, lane, peer, src=None):
        ref = place(k, slot)
        return pltpu.make_async_remote_copy(
            src_ref=ref if src is None else src, dst_ref=ref,
            send_sem=ssem.at[k, lane, slot], recv_sem=rsem.at[k, slot],
            device_id=peer, device_id_type=MESH,
        )

    UP, DOWN, YY, CC = range(4)
    for k in range(3):
        @pl.when(z < last)
        def _():
            copy(k, me, UP, up, own[k]).start()

        @pl.when(z > 0)
        def _():
            copy(k, me, DOWN, down, own[k]).start()

        copy(k, me, YY, y_peer, own[k]).start()
        copy(k, me, CC, c_peer, own[k]).start()

    gx[me] = g_ref[...]
    tx[pl.ds(pl.multiple_of(me * tok, tok), tok), :] = x_ref[...]
    ty[pl.ds(pl.multiple_of(me * tok, tok), tok), :] = dy_ref[...]

    t_y = (1 - y) * 2 + c
    t_c = y * 2 + (1 - c)
    t_yc = (1 - y) * 2 + (1 - c)

    def from_y(slot):
        for k in range(3):
            copy(k, slot, CC, c_peer).wait_recv()
            copy(k, slot, CC, c_peer).start()

    def level(d):
        for k in range(3):
            @pl.when(z - d >= 0)
            def _():
                slot = (z - d) * 4 + t
                copy(k, slot, UP, up).wait_recv()

                @pl.when(z < last)
                def _():
                    copy(k, slot, UP, up).start()

                copy(k, slot, YY, y_peer).start()
                copy(k, slot, CC, c_peer).start()

            @pl.when(z + d <= last)
            def _():
                slot = (z + d) * 4 + t
                copy(k, slot, DOWN, down).wait_recv()

                @pl.when(z > 0)
                def _():
                    copy(k, slot, DOWN, down).start()

                copy(k, slot, YY, y_peer).start()
                copy(k, slot, CC, c_peer).start()

    def y_level(d):
        @pl.when(z - d >= 0)
        def _():
            from_y((z - d) * 4 + t_y)

        @pl.when(z + d <= last)
        def _():
            from_y((z + d) * 4 + t_y)

    level(1)
    from_y(z * 4 + t_y)
    level(2)
    y_level(1)
    level(3)
    y_level(2)
    y_level(3)

    for zz in range(4):
        for tt in (t_c, t_yc):
            for k in range(3):
                copy(k, zz * 4 + tt, CC, c_peer).wait_recv()

    for zz in range(4):
        for k in range(3):
            slot = zz * 4 + t
            copy(k, slot, YY, y_peer).wait_send()
            copy(k, slot, CC, c_peer).wait_send()
            copy(k, zz * 4 + t_y, CC, c_peer).wait_send()

            @pl.when((zz <= z) & (z < last))
            def _():
                copy(k, slot, UP, up).wait_send()

            @pl.when((zz >= z) & (z > 0))
            def _():
                copy(k, slot, DOWN, down).wait_send()


def grad_kernel(u_hbm, v_hbm, tx, ty, gx, du_hbm, dv_hbm, ru_out, rv_out,
                zbuf, ugrp, vgrp, uacc, vacc, rows_u, rows_v, pu, pv, vslot, sslot,
                zsem, gsem, ssem, psem):
    z = lax.axis_index("data")
    r = lax.axis_index("table")
    n_local, width = u_hbm.shape
    n_ent = rows_u.shape[0]
    zrows = zbuf.shape[0]
    zbuf[...] = jnp.zeros_like(zbuf)

    ids = jnp.concatenate([gx[e, 64:65, :] for e in range(16)], axis=0)
    pick = ids[:, 0:32]
    for o in range(1, 4):
        pick = jnp.where(r == o, ids[:, o * 32 : o * 32 + 32], pick)
    pick = pick - (r * n_local).astype(F32)
    idrow = jnp.concatenate([pick[e : e + 1, :] for e in range(16)], axis=1)
    ii = lax.broadcasted_iota(jnp.int32, (n_ent, n_ent), 0)
    jj = lax.broadcasted_iota(jnp.int32, (n_ent, n_ent), 1)

    def lanes(cond, val):
        return jnp.sum(jnp.where(cond, val, 0.0), axis=1, keepdims=True)

    def subl(cond, val):
        return jnp.sum(jnp.where(cond, val, 0.0), axis=0, keepdims=True)

    idcol = lanes(ii == jj, jnp.broadcast_to(idrow, (n_ent, n_ent)))
    grow, gcol = jnp.floor(idrow * 0.125), jnp.floor(idcol * 0.125)
    same = gcol == grow
    lead_col = jnp.where(lanes(same & (jj < ii), 1.0) == 0.0, 1.0, 0.0)
    lead_row = jnp.where(subl(same & (ii < jj), 1.0) == 0.0, 1.0, 0.0)
    rank_col = lanes(jj < ii, jnp.broadcast_to(lead_row, (n_ent, n_ent)))
    rank_row = subl(ii < jj, jnp.broadcast_to(lead_col, (n_ent, n_ent)))
    hit_c = (rank_col.astype(jnp.int32) == jj) & (lead_col > 0.0)
    hit_r = (rank_row.astype(jnp.int32) == ii) & (lead_row > 0.0)
    count = jnp.sum(lead_row, axis=1, keepdims=True)
    slot_row = subl(hit_c, jnp.broadcast_to(gcol, (n_ent, n_ent)))
    slot_col = lanes(hit_r, jnp.broadcast_to(grow, (n_ent, n_ent)))
    lane_id = lax.broadcasted_iota(jnp.int32, (1, n_ent), 1)
    sub_id = lax.broadcasted_iota(jnp.int32, (n_ent, 1), 0)
    icount = count.astype(jnp.int32)
    vslot[0:1, :] = slot_row.astype(jnp.int32)
    vslot[1:2, :] = jnp.broadcast_to(icount, (1, n_ent))
    slot_row = jnp.where(lane_id < icount, slot_row, -1.0)
    slot_col = jnp.where(sub_id < icount, slot_col, -1.0)

    def fill(i, table, k):
        return pltpu.make_async_copy(zbuf, table.at[pl.ds(i * zrows, zrows), :], zsem.at[k])

    for i in range(n_local // zrows):
        fill(i, du_hbm, 0).start()
        fill(i, dv_hbm, 1).start()
    to_smem = pltpu.make_async_copy(vslot, sslot, ssem)
    to_smem.start()
    to_smem.wait()
    n_slot = sslot[1, 0]
    n_blk = (n_slot + 31) // 32

    def fetch(k, table, grp, s):
        g = pl.multiple_of(sslot[0, k] * 8, 8)
        return pltpu.make_async_copy(table.at[pl.ds(g, 8), :], grp.at[pl.ds(pl.multiple_of(k * 8, 8), 8), :], gsem.at[s])

    def start_fetch(k, carry):
        fetch(k, u_hbm, ugrp, 0).start()
        fetch(k, v_hbm, vgrp, 1).start()
        return carry

    def wait_fetch(k, carry):
        fetch(k, u_hbm, ugrp, 0).wait()
        fetch(k, v_hbm, vgrp, 1).wait()
        return carry

    lax.fori_loop(0, n_blk * 32, start_fetch, 0)
    lax.fori_loop(0, n_blk * 32, wait_fetch, 0)

    qrow = lax.broadcasted_iota(jnp.int32, (1, 256), 1)
    qcol = lax.broadcasted_iota(jnp.int32, (256, 1), 0)
    uacc[...] = jnp.zeros_like(uacc)
    vacc[...] = jnp.zeros_like(vacc)
    kk = lax.broadcasted_iota(jnp.int32, (n_ent, 256), 0)
    qk = lax.broadcasted_iota(jnp.int32, (n_ent, 256), 1) >> 3

    def take_rows(b, carry):
        rowid = 8.0 * subl(kk == qk + b * 32, jnp.broadcast_to(slot_col, (n_ent, 256))) + (qrow & 7).astype(F32)
        pickm = jnp.where(idcol == rowid, 1.0, 0.0).astype(BF16)
        base = pl.multiple_of(b * 256, 256)
        uacc[...] += dot(pickm, ugrp[pl.ds(base, 256), :])
        vacc[...] += dot(pickm, vgrp[pl.ds(base, 256), :])
        return carry

    lax.fori_loop(0, n_blk, take_rows, 0)
    rows_u[...] = uacc[...].astype(BF16)
    rows_v[...] = vacc[...].astype(BF16)
    mine = pl.ds(pl.multiple_of(z * 128, 128), 128)
    ru_out[...] = rows_u[mine, :]
    rv_out[...] = rows_v[mine, :]

    diag = (lax.broadcasted_iota(jnp.int32, (128, 256), 0) >> 5) == (lax.broadcasted_iota(jnp.int32, (128, 256), 1) >> 6)
    for d in range(4):
        x4, dy4 = tx[256 * d : 256 * d + 256, :], ty[256 * d : 256 * d + 256, :]
        u4, v4 = rows_u[128 * d : 128 * d + 128, :], rows_v[128 * d : 128 * d + 128, :]
        gates = []
        for e in range(4 * d, 4 * d + 4):
            part = gx[e, pl.ds(pl.multiple_of(lax.rem(r, 2) * 32, 32), 32), :]
            part = jnp.where(r >= 2, part[:, 64:128], part[:, 0:64])
            gates.append(jnp.concatenate([part] * 4, axis=1))
        g4 = jnp.concatenate(gates, axis=0)
        act, slope = gelu_pair(dot(u4, x4, NT))
        b4 = dot(v4, dy4, NT)
        w4 = jnp.where(diag, g4 * act, 0.0)
        c4 = jnp.where(diag, g4 * slope * b4, 0.0)
        for coef, val, out in ((c4, x4, pu), (w4, dy4, pv)):
            full = dot(jnp.concatenate(split3(coef), axis=0), val)
            full = full[0:128] + full[128:256] + full[256:384]
            for k, term in enumerate(split3(full)):
                out[k, 128 * d : 128 * d + 128, :] = term

    kq = lax.broadcasted_iota(jnp.int32, (256, n_ent), 1)
    qq = lax.broadcasted_iota(jnp.int32, (256, n_ent), 0) >> 3

    def put_rows(b, carry):
        rowid = 8.0 * lanes(kq == qq + b * 32, jnp.broadcast_to(slot_row, (256, n_ent))) + (qcol & 7).astype(F32)
        spread = jnp.where(rowid == idrow, 1.0, 0.0).astype(BF16)
        base = pl.multiple_of(b * 256, 256)
        ugrp[pl.ds(base, 256), :] = (dot(spread, pu[0]) + dot(spread, pu[1]) + dot(spread, pu[2])).astype(BF16)
        vgrp[pl.ds(base, 256), :] = (dot(spread, pv[0]) + dot(spread, pv[1]) + dot(spread, pv[2])).astype(BF16)
        return carry

    lax.fori_loop(0, n_blk, put_rows, 0)
    for i in range(n_local // zrows):
        fill(i, du_hbm, 0).wait()
        fill(i, dv_hbm, 1).wait()

    def patch(k, table, grp, s):
        g = pl.multiple_of(sslot[0, k] * 8, 8)
        return pltpu.make_async_copy(grp.at[pl.ds(pl.multiple_of(k * 8, 8), 8), :], table.at[pl.ds(g, 8), :], psem.at[s])

    def start_patch(k, carry):
        patch(k, du_hbm, ugrp, 0).start()
        patch(k, dv_hbm, vgrp, 1).start()
        return carry

    def wait_patch(k, carry):
        patch(k, du_hbm, ugrp, 0).wait()
        patch(k, dv_hbm, vgrp, 1).wait()
        return carry

    lax.fori_loop(0, n_slot, start_patch, 0)
    lax.fori_loop(0, n_slot, wait_patch, 0)


def token_kernel(ru, rv, x_ref, dy_ref, g_ref, y_out, dx_out, ubuf, vbuf, ssem, rsem):
    r = lax.axis_index("table")
    bar = pltpu.get_barrier_semaphore()
    for s in range(1, 4):
        pl.semaphore_signal(bar, inc=1, device_id={"table": lax.rem(r + s, 4)}, device_id_type=MESH)
    pl.semaphore_wait(bar, 3)
    mine = pl.ds(pl.multiple_of(r * 32, 32), 32)

    def send(k, s):
        to = lax.rem(r + s, 4)
        return pltpu.make_async_remote_copy(
            src_ref=(ru, rv)[k].at[pl.ds(pl.multiple_of(to * 32, 32), 32), :],
            dst_ref=(ubuf, vbuf)[k].at[mine, :],
            send_sem=ssem.at[k, s], recv_sem=rsem.at[k, s],
            device_id={"table": to}, device_id_type=MESH,
        )

    for k in range(2):
        for s in (2, 1, 3):
            send(k, s).start()
    ubuf[mine, :] = ru[mine, :]
    vbuf[mine, :] = rv[mine, :]
    gates = jnp.concatenate([g_ref[0:64, 0:64], g_ref[0:64, 64:128]], axis=0)
    for s in range(1, 4):
        send(0, s).wait_recv()
    act, slope = gelu_pair(dot(ubuf[...], x_ref[...], NT))
    for s in range(1, 4):
        send(1, s).wait_recv()
    b_val = dot(vbuf[...], dy_ref[...], NT)
    w_val = jnp.transpose(gates * act)
    c_val = jnp.transpose(gates * slope * b_val)
    for coef, rows, out in ((w_val, vbuf, y_out), (c_val, ubuf, dx_out)):
        full = dot(jnp.concatenate(split3(coef), axis=0), rows[...])
        out[...] = (full[0:64] + full[64:128] + full[128:192]).astype(BF16)
    for k in range(2):
        for s in range(1, 4):
            send(k, s).wait_send()


def solution(mesh):
    tok_spec = P(('replica', 'data', 'table'))
    row_spec = P(('replica', 'table'))

    def device_step(tok, dy, u, v, wanted, pick, gate):
        n_tok, width = tok.shape
        n_local = u.shape[0]
        sel = pick.shape[1] * pick.shape[2]
        pick_t = jnp.transpose(pick, (1, 2, 0)).reshape(sel, n_tok)
        gate_t = jnp.transpose(gate, (1, 2, 0)).reshape(sel, n_tok)
        shape = jax.ShapeDtypeStruct
        g_own = pl.pallas_call(
            gate_kernel, out_shape=shape((72, 128), F32), in_specs=[VMEM] * 3, out_specs=VMEM,
        )(pick_t, gate_t, wanted)
        tx, ty, gx = pl.pallas_call(
            share_kernel,
            out_shape=[shape((16 * n_tok, width), BF16)] * 2 + [shape((16, 72, 128), F32)],
            in_specs=[VMEM] * 3, out_specs=[VMEM] * 3,
            scratch_shapes=[pltpu.SemaphoreType.DMA((3, 4, 16)), pltpu.SemaphoreType.DMA((3, 16))],
            compiler_params=pltpu.CompilerParams(collective_id=0, has_side_effects=True),
        )(tok, dy, g_own)
        du, dv, ru, rv = pl.pallas_call(
            grad_kernel,
            out_shape=[shape((n_local, width), BF16)] * 2 + [shape((128, width), BF16)] * 2,
            in_specs=[ANY, ANY, VMEM, VMEM, VMEM], out_specs=[ANY, ANY, VMEM, VMEM],
            scratch_shapes=[
                pltpu.VMEM((512, width), BF16), pltpu.VMEM((4096, width), BF16), pltpu.VMEM((4096, width), BF16),
                pltpu.VMEM((512, width), F32), pltpu.VMEM((512, width), F32),
                pltpu.VMEM((512, width), BF16), pltpu.VMEM((512, width), BF16),
                pltpu.VMEM((3, 512, width), BF16), pltpu.VMEM((3, 512, width), BF16),
                pltpu.VMEM((8, 512), jnp.int32), pltpu.SMEM((8, 512), jnp.int32),
                pltpu.SemaphoreType.DMA((2,)), pltpu.SemaphoreType.DMA((2,)),
                pltpu.SemaphoreType.DMA, pltpu.SemaphoreType.DMA((2,)),
            ],
            compiler_params=pltpu.CompilerParams(vmem_limit_bytes=BIG),
        )(u, v, tx, ty, gx)
        y, dx = pl.pallas_call(
            token_kernel,
            out_shape=[shape((n_tok, width), BF16)] * 2,
            in_specs=[VMEM] * 5, out_specs=[VMEM] * 2,
            scratch_shapes=[
                pltpu.VMEM((128, width), BF16), pltpu.VMEM((128, width), BF16),
                pltpu.SemaphoreType.DMA((2, 4)), pltpu.SemaphoreType.DMA((2, 4)),
            ],
            compiler_params=pltpu.CompilerParams(collective_id=1, has_side_effects=True),
        )(ru, rv, tok, dy, g_own)
        return y, dx, du, dv

    return jax.shard_map(device_step, mesh=mesh, in_specs=(tok_spec, tok_spec, row_spec, row_spec, tok_spec, tok_spec, tok_spec), out_specs=(tok_spec, tok_spec, row_spec, row_spec), check_vma=False)
```

```python
import functools

import jax
import jax.numpy as jnp
from jax import lax
from jax.experimental import pallas as pl
from jax.experimental.pallas import tpu as pltpu
from jax.sharding import PartitionSpec as P

MESH = pl.DeviceIdType.MESH
F32 = jnp.float32
BF16 = jnp.bfloat16
VMEM = pl.BlockSpec(memory_space=pltpu.VMEM)
ANY = pl.BlockSpec(memory_space=pl.ANY)
NT = (((1,), (1,)), ((), ()))
TN = (((0,), (0,)), ((), ()))
HBM = pl.BlockSpec(memory_space=pltpu.HBM)
SMEM = pl.BlockSpec(memory_space=pltpu.SMEM)
MB = 1024 * 1024
UP, DOWN, YY, CC = range(4)


def gelu_pair(pre_act):
    cdf_val = 0.5 * (1.0 + lax.erf(pre_act * 0.7071067811865476))
    pdf_val = jnp.exp(-0.5 * pre_act * pre_act) * 0.3989422804014327
    return pre_act * cdf_val, cdf_val + pre_act * pdf_val


def split3(val):
    one = val.astype(BF16)
    rest = val - one.astype(F32)
    two = rest.astype(BF16)
    three = (rest - two.astype(F32)).astype(BF16)
    return one, two, three


def dot(a, b, dims=None):
    if dims is None:
        return jnp.dot(a, b, preferred_element_type=F32)
    return lax.dot_general(a, b, dims, preferred_element_type=F32)


def ids_kernel(ids_ref, out, ssem, rsem):
    z = lax.axis_index("data")
    t = lax.axis_index("table")
    me = z * 4 + t
    bar = pltpu.get_barrier_semaphore()
    peers = [(lax.rem(z + dz, 4), lax.rem(t + dt, 4)) for dz in range(4) for dt in range(4)][1:]
    for pz, pt in peers:
        pl.semaphore_signal(bar, inc=1, device_id={"data": pz, "table": pt}, device_id_type=MESH)
    pl.semaphore_wait(bar, 15)
    copies = []
    for i, (pz, pt) in enumerate(peers):
        copies.append(pltpu.make_async_remote_copy(
            src_ref=ids_ref, dst_ref=out.at[me], send_sem=ssem.at[i], recv_sem=rsem.at[i],
            device_id={"data": pz, "table": pt}, device_id_type=MESH,
        ))
        copies[-1].start()
    out[me] = ids_ref[...]
    for one in copies:
        one.wait()


def prep_kernel(u_hbm, v_hbm, pick_ref, gate_ref, ids_ref, du_hbm, dv_hbm, g_out, rows_u, rows_v, vslot, meta,
                zbuf, ugrp, vgrp, uacc, vacc, sslot, zsem, gsem, ssem):
    r = lax.axis_index("table")
    n_local = u_hbm.shape[0]
    n_ent = rows_u.shape[0]
    zrows = zbuf.shape[0]
    zbuf[...] = jnp.zeros_like(zbuf)

    ids = jnp.concatenate([ids_ref[e] for e in range(16)], axis=0).astype(F32)
    pick = ids[:, 0:32]
    for o in range(1, 4):
        pick = jnp.where(r == o, ids[:, o * 32 : o * 32 + 32], pick)
    pick = pick - (r * n_local).astype(F32)
    idrow = jnp.concatenate([pick[e : e + 1, :] for e in range(16)], axis=1)
    ii = lax.broadcasted_iota(jnp.int32, (n_ent, n_ent), 0)
    jj = lax.broadcasted_iota(jnp.int32, (n_ent, n_ent), 1)

    def fill(i, table, k):
        return pltpu.make_async_copy(zbuf, table.at[pl.ds(i * zrows, zrows), :], zsem.at[k])

    for i in range(n_local // zrows):
        fill(i, du_hbm, 0).start()
        fill(i, dv_hbm, 1).start()

    def lanes(cond, val):
        return jnp.sum(jnp.where(cond, val, 0.0), axis=1, keepdims=True)

    def subl(cond, val):
        return jnp.sum(jnp.where(cond, val, 0.0), axis=0, keepdims=True)

    idcol = lanes(ii == jj, jnp.broadcast_to(idrow, (n_ent, n_ent)))
    grow, gcol = jnp.floor(idrow * 0.125), jnp.floor(idcol * 0.125)
    same = gcol == grow
    lead_col = jnp.where(lanes(same & (jj < ii), 1.0) == 0.0, 1.0, 0.0)
    lead_row = jnp.where(subl(same & (ii < jj), 1.0) == 0.0, 1.0, 0.0)
    rank_col = lanes(jj < ii, jnp.broadcast_to(lead_row, (n_ent, n_ent)))
    rank_row = subl(ii < jj, jnp.broadcast_to(lead_col, (n_ent, n_ent)))
    hit_c = (rank_col.astype(jnp.int32) == jj) & (lead_col > 0.0)
    hit_r = (rank_row.astype(jnp.int32) == ii) & (lead_row > 0.0)
    icount = jnp.sum(lead_row, axis=1, keepdims=True).astype(jnp.int32)
    slot_row = subl(hit_c, jnp.broadcast_to(gcol, (n_ent, n_ent)))
    slot_col = lanes(hit_r, jnp.broadcast_to(grow, (n_ent, n_ent)))
    vslot[0:1, :] = slot_row.astype(jnp.int32)
    vslot[1:8, :] = jnp.broadcast_to(icount, (7, n_ent))
    slot_row = jnp.where(jj[0:1, :] < icount, slot_row, -1.0)
    slot_col = jnp.where(ii[:, 0:1] < icount, slot_col, -1.0)
    meta[0:1, :] = idrow
    meta[1:8, :] = jnp.broadcast_to(slot_row, (7, n_ent))

    sel, tok = pick_ref.shape
    half = sel // 2
    row = lax.broadcasted_iota(jnp.int32, (half, 2 * tok), 0)

    def add_gates(i, acc):
        base = pl.multiple_of(i * 8, 8)
        pick8 = pick_ref[pl.ds(base, 8), :]
        gate8 = gate_ref[pl.ds(base, 8), :]
        pick8 = jnp.concatenate([pick8, pick8 - half], axis=1)
        gate8 = jnp.concatenate([gate8, gate8], axis=1)
        for j in range(8):
            acc = acc + jnp.where(row == pick8[j : j + 1, :], gate8[j : j + 1, :], 0.0)
        return acc

    g_out[...] = lax.fori_loop(0, sel // 8, add_gates, jnp.zeros((half, 2 * tok), F32))

    to_smem = pltpu.make_async_copy(vslot, sslot, ssem)
    to_smem.start()
    to_smem.wait()
    n_blk = (sslot[1, 0] + 31) // 32

    def fetch(k, table, grp, s):
        g = pl.multiple_of(sslot[0, k] * 8, 8)
        return pltpu.make_async_copy(table.at[pl.ds(g, 8), :], grp.at[pl.ds(pl.multiple_of(k * 8, 8), 8), :], gsem.at[s])

    def start_fetch(k, carry):
        fetch(k, u_hbm, ugrp, 0).start()
        fetch(k, v_hbm, vgrp, 1).start()
        return carry

    def wait_fetch(k, carry):
        fetch(k, u_hbm, ugrp, 0).wait()
        fetch(k, v_hbm, vgrp, 1).wait()
        return carry

    lax.fori_loop(0, n_blk * 32, start_fetch, 0)
    lax.fori_loop(0, n_blk * 32, wait_fetch, 0)

    uacc[...] = jnp.zeros_like(uacc)
    vacc[...] = jnp.zeros_like(vacc)
    kk = lax.broadcasted_iota(jnp.int32, (n_ent, 256), 0)
    qk = lax.broadcasted_iota(jnp.int32, (n_ent, 256), 1) >> 3
    q7 = (lax.broadcasted_iota(jnp.int32, (1, 256), 1) & 7).astype(F32)

    def take_rows(b, carry):
        rowid = 8.0 * subl(kk == qk + b * 32, jnp.broadcast_to(slot_col, (n_ent, 256))) + q7
        pickm = jnp.where(idcol == rowid, 1.0, 0.0).astype(BF16)
        base = pl.multiple_of(b * 256, 256)
        uacc[...] += dot(pickm, ugrp[pl.ds(base, 256), :])
        vacc[...] += dot(pickm, vgrp[pl.ds(base, 256), :])
        return carry

    lax.fori_loop(0, n_blk, take_rows, 0)
    rows_u[...] = uacc[...].astype(BF16)
    rows_v[...] = vacc[...].astype(BF16)
    for i in range(n_local // zrows):
        fill(i, du_hbm, 0).wait()
        fill(i, dv_hbm, 1).wait()


def main_kernel(x_ref, dy_ref, g_ref, xd, dyd, xu, dyu, xy, dyy, ru, rv, pu, pv, y_out, dx_out,
                tx, ty, gx, ubuf, vbuf, ssem, rsem, rows_s, rows_r):
    z = lax.axis_index("data")
    t = lax.axis_index("table")
    last = 3
    y, c = t // 2, lax.rem(t, 2)
    t_y = (1 - y) * 2 + c
    t_c = y * 2 + (1 - c)
    t_yc = (1 - y) * 2 + (1 - c)
    y_peer, c_peer = {"table": t_y}, {"table": t_c}
    up, down = {"data": z + 1}, {"data": z - 1}
    tok = x_ref.shape[0]

    bar = pltpu.get_barrier_semaphore()
    for peer in (t_y, t_c, t_yc):
        pl.semaphore_signal(bar, inc=1, device_id={"table": peer}, device_id_type=MESH)

    @pl.when(z < last)
    def _():
        pl.semaphore_signal(bar, inc=1, device_id=up, device_id_type=MESH)

    @pl.when(z > 0)
    def _():
        pl.semaphore_signal(bar, inc=1, device_id=down, device_id_type=MESH)

    pl.semaphore_wait(bar, 3 + (z < last).astype(jnp.int32) + (z > 0).astype(jnp.int32))

    outs = (gx, tx, ty)
    GATE, TOKS = (0,), (1, 2)

    def place(k, slot):
        if k == 0:
            return gx.at[slot]
        return outs[k].at[pl.ds(pl.multiple_of(slot * tok, tok), tok), :]

    def copy(k, slot, lane, peer, src=None):
        ref = place(k, slot)
        return pltpu.make_async_remote_copy(
            src_ref=ref if src is None else src, dst_ref=ref,
            send_sem=ssem.at[k, lane, slot], recv_sem=rsem.at[k, slot],
            device_id=peer, device_id_type=MESH,
        )

    def zslot(d):
        return (z + d) * 4 + t

    def send_row(k, s):
        to = lax.rem(t + s, 4)
        return pltpu.make_async_remote_copy(
            src_ref=(ru, rv)[k].at[pl.ds(pl.multiple_of(z * 128 + to * 32, 32), 32), :],
            dst_ref=(ubuf, vbuf)[k].at[pl.ds(pl.multiple_of(t * 32, 32), 32), :],
            send_sem=rows_s.at[k, s], recv_sem=rows_r.at[k, s],
            device_id={"table": to}, device_id_type=MESH,
        )

    own = (g_ref, x_ref, dy_ref)
    low = (None, xd, dyd)
    high = (None, xu, dyu)
    across = (None, xy, dyy)
    me = zslot(0)

    @pl.when(z < last)
    def _():
        copy(0, me, UP, up, g_ref).start()

    @pl.when(z > 0)
    def _():
        copy(0, me, DOWN, down, g_ref).start()

    copy(0, me, YY, y_peer, g_ref).start()
    copy(0, me, CC, c_peer, g_ref).start()

    for k in TOKS:
        @pl.when(z > 0)
        def _():
            @pl.when(z < last)
            def _():
                copy(k, zslot(-1), UP, up, low[k]).start()

            copy(k, zslot(-1), YY, y_peer, low[k]).start()

        @pl.when(z < last)
        def _():
            @pl.when(z > 0)
            def _():
                copy(k, zslot(1), DOWN, down, high[k]).start()

            copy(k, zslot(1), YY, y_peer, high[k]).start()

    for k in range(2):
        for s in (2, 1, 3):
            send_row(k, s).start()

    for k in TOKS:
        copy(k, me, CC, c_peer, own[k]).start()
        copy(k, z * 4 + t_y, CC, c_peer, across[k]).start()

        @pl.when(z > 0)
        def _():
            copy(k, zslot(-1), CC, c_peer, low[k]).start()

        @pl.when(z < last)
        def _():
            copy(k, zslot(1), CC, c_peer, high[k]).start()

    gx[me] = g_ref[...]
    for k in TOKS:
        outs[k][pl.ds(pl.multiple_of(me * tok, tok), tok), :] = own[k][...]
        outs[k][pl.ds(pl.multiple_of((z * 4 + t_y) * tok, tok), tok), :] = across[k][...]

        @pl.when(z > 0)
        def _():
            outs[k][pl.ds(pl.multiple_of(zslot(-1) * tok, tok), tok), :] = low[k][...]

        @pl.when(z < last)
        def _():
            outs[k][pl.ds(pl.multiple_of(zslot(1) * tok, tok), tok), :] = high[k][...]

    mine = pl.ds(pl.multiple_of(t * 32, 32), 32)
    ubuf[mine, :] = ru[pl.ds(pl.multiple_of(z * 128 + t * 32, 32), 32), :]
    vbuf[mine, :] = rv[pl.ds(pl.multiple_of(z * 128 + t * 32, 32), 32), :]

    def level(d, ks):
        for k in ks:
            @pl.when(z - d >= 0)
            def _():
                slot = zslot(-d)
                copy(k, slot, UP, up).wait_recv()

                @pl.when(z < last)
                def _():
                    copy(k, slot, UP, up).start()

                copy(k, slot, YY, y_peer).start()
                copy(k, slot, CC, c_peer).start()

            @pl.when(z + d <= last)
            def _():
                slot = zslot(d)
                copy(k, slot, DOWN, down).wait_recv()

                @pl.when(z > 0)
                def _():
                    copy(k, slot, DOWN, down).start()

                copy(k, slot, YY, y_peer).start()
                copy(k, slot, CC, c_peer).start()

    def from_y(slot, ks):
        for k in ks:
            copy(k, slot, CC, c_peer).wait_recv()
            copy(k, slot, CC, c_peer).start()

    def y_level(d, ks):
        @pl.when(z - d >= 0)
        def _():
            from_y((z - d) * 4 + t_y, ks)

        @pl.when(z + d <= last)
        def _():
            from_y((z + d) * 4 + t_y, ks)

    diag = (lax.broadcasted_iota(jnp.int32, (128, 256), 0) >> 5) == (lax.broadcasted_iota(jnp.int32, (128, 256), 1) >> 6)

    def products(d):
        for tt in (t_c, t_yc):
            for k in range(3):
                copy(k, d * 4 + tt, CC, c_peer).wait_recv()
        tsl = pl.ds(pl.multiple_of(d * 256, 256), 256)
        esl = pl.ds(pl.multiple_of(d * 128, 128), 128)
        x4, dy4 = tx[tsl, :], ty[tsl, :]
        u4, v4 = ru[esl, :], rv[esl, :]
        gates = []
        for e in range(4):
            part = gx[d * 4 + e, pl.ds(pl.multiple_of(c * 32, 32), 32), :]
            part = jnp.where(y == 1, part[:, 64:128], part[:, 0:64])
            gates.append(jnp.concatenate([part] * 4, axis=1))
        g4 = jnp.concatenate(gates, axis=0)
        act, slope = gelu_pair(dot(u4, x4, NT))
        b4 = dot(v4, dy4, NT)
        w4 = jnp.where(diag, g4 * act, 0.0)
        c4 = jnp.where(diag, g4 * slope * b4, 0.0)
        for coef, val, out in ((c4, x4, pu), (w4, dy4, pv)):
            full = dot(jnp.concatenate(split3(coef), axis=0), val)
            full = full[0:128] + full[128:256] + full[256:384]
            for k, term in enumerate(split3(full)):
                out[k, esl, :] = term

    def products_at(d):
        @pl.when(z - d >= 0)
        def _():
            products(z - d)

        @pl.when(z + d <= last)
        def _():
            products(z + d)

    level(1, GATE)
    from_y(z * 4 + t_y, GATE)
    level(2, GATE)
    y_level(1, GATE)
    products(z)
    level(2, TOKS)
    level(3, GATE)
    y_level(2, GATE)
    y_level(3, GATE)
    y_level(1, TOKS)
    level(3, TOKS)

    gates = jnp.concatenate([g_ref[:, 0:64], g_ref[:, 64:128]], axis=0)
    for s in range(1, 4):
        send_row(0, s).wait_recv()
        send_row(1, s).wait_recv()
    act, slope = gelu_pair(dot(ubuf[...], x_ref[...], NT))
    b_val = dot(vbuf[...], dy_ref[...], NT)
    w_val = jnp.transpose(gates * act)
    c_val = jnp.transpose(gates * slope * b_val)
    for coef, rows, out in ((w_val, vbuf, y_out), (c_val, ubuf, dx_out)):
        full = dot(jnp.concatenate(split3(coef), axis=0), rows[...])
        out[...] = (full[0:64] + full[64:128] + full[128:192]).astype(BF16)

    products_at(1)
    y_level(2, TOKS)
    y_level(3, TOKS)
    products_at(2)
    products_at(3)

    for k in range(2):
        for s in range(1, 4):
            send_row(k, s).wait_send()
    for zz in range(4):
        slot = zz * 4 + t
        for k in range(3):
            copy(k, slot, CC, c_peer).wait_send()
            copy(k, zz * 4 + t_y, CC, c_peer).wait_send()
            if k == 0:
                copy(k, slot, YY, y_peer).wait_send()
                sent_up, sent_down = zz <= z, zz >= z
            else:
                @pl.when(zz != z)
                def _():
                    copy(k, slot, YY, y_peer).wait_send()

                sent_up, sent_down = zz < z, zz > z

            @pl.when(sent_up & (z < last))
            def _():
                copy(k, slot, UP, up).wait_send()

            @pl.when(sent_down & (z > 0))
            def _():
                copy(k, slot, DOWN, down).wait_send()


def put_kernel(pu, pv, y_ref, dx_ref, sslot, meta, du_in, dv_in, du_hbm, dv_hbm, y_out, dx_out, ures, vres, psem):
    n_ent = pu.shape[1]
    y_out[...] = y_ref[...]
    dx_out[...] = dx_ref[...]
    n_slot = sslot[1, 0]
    n_blk = (n_slot + 31) // 32
    idrow, slot_row = meta[0:1, :], meta[1:2, :]
    kq = lax.broadcasted_iota(jnp.int32, (256, n_ent), 1)
    qq = lax.broadcasted_iota(jnp.int32, (256, n_ent), 0) >> 3
    q7 = (lax.broadcasted_iota(jnp.int32, (256, 1), 0) & 7).astype(F32)

    def patch(k, table, res, s):
        g = pl.multiple_of(sslot[0, k] * 8, 8)
        return pltpu.make_async_copy(res.at[pl.ds(pl.multiple_of(k * 8, 8), 8), :], table.at[pl.ds(g, 8), :], psem.at[s])

    def put_rows(b, carry):
        rowid = 8.0 * jnp.sum(jnp.where(kq == qq + b * 32, slot_row, 0.0), axis=1, keepdims=True) + q7
        spread = jnp.where(rowid == idrow, 1.0, 0.0).astype(BF16)
        base = pl.multiple_of(b * 256, 256)
        ures[pl.ds(base, 256), :] = (dot(spread, pu[0]) + dot(spread, pu[1]) + dot(spread, pu[2])).astype(BF16)
        vres[pl.ds(base, 256), :] = (dot(spread, pv[0]) + dot(spread, pv[1]) + dot(spread, pv[2])).astype(BF16)
        return carry

    lax.fori_loop(0, n_blk, put_rows, 0)

    def start_patch(k, carry):
        patch(k, du_hbm, ures, 0).start()
        patch(k, dv_hbm, vres, 1).start()
        return carry

    def wait_patch(k, carry):
        patch(k, du_hbm, ures, 0).wait()
        patch(k, dv_hbm, vres, 1).wait()
        return carry

    lax.fori_loop(0, n_slot, start_patch, 0)
    lax.fori_loop(0, n_slot, wait_patch, 0)


def solution(mesh):
    tok_spec = P(('replica', 'data', 'table'))
    row_spec = P(('replica', 'table'))

    def device_step(tok, dy, u, v, wanted, pick, gate):
        n_tok, width = tok.shape
        n_local = u.shape[0]
        sel = pick.shape[1] * pick.shape[2]
        shape = jax.ShapeDtypeStruct
        dma = pltpu.SemaphoreType.DMA
        rows = shape((512, width), BF16)
        block = shape((n_tok, width), BF16)
        table = shape((n_local, width), BF16)
        pick_t = jnp.transpose(pick, (1, 2, 0)).reshape(sel, n_tok)
        gate_t = jnp.transpose(gate, (1, 2, 0)).reshape(sel, n_tok)

        def hop(axis, pairs):
            return [lax.ppermute(val, axis, pairs) for val in (tok, dy)]

        xd, dyd = hop('data', [(0, 1), (1, 2), (2, 3)])
        xu, dyu = hop('data', [(1, 0), (2, 1), (3, 2)])
        xy, dyy = hop('table', [(0, 2), (1, 3), (2, 0), (3, 1)])
        ids = pl.pallas_call(
            ids_kernel, out_shape=shape((16, 1, 128), jnp.int32), in_specs=[VMEM], out_specs=VMEM,
            scratch_shapes=[dma((15,)), dma((15,))],
            compiler_params=pltpu.CompilerParams(collective_id=0, has_side_effects=True, vmem_limit_bytes=4 * MB),
            cost_estimate=pl.CostEstimate(flops=int(5e8), bytes_accessed=10000, transcendentals=0),
        )(wanted)
        du, dv, g_own, ru, rv, vslot, meta = pl.pallas_call(
            prep_kernel,
            out_shape=[table, table, shape((64, 128), F32), rows, rows, shape((8, 512), jnp.int32), shape((8, 512), F32)],
            in_specs=[HBM, HBM, VMEM, VMEM, VMEM], out_specs=[HBM, HBM] + [VMEM] * 5,
            scratch_shapes=[
                pltpu.VMEM((512, width), BF16), pltpu.VMEM((4096, width), BF16), pltpu.VMEM((4096, width), BF16),
                pltpu.VMEM((512, width), F32), pltpu.VMEM((512, width), F32),
                pltpu.SMEM((8, 512), jnp.int32), dma((2,)), dma((2,)), dma,
            ],
            compiler_params=pltpu.CompilerParams(vmem_limit_bytes=36 * MB),
            cost_estimate=pl.CostEstimate(flops=int(8e9), bytes_accessed=60 * MB, transcendentals=0),
        )(u, v, pick_t, gate_t, ids)
        pu, pv, y, dx = pl.pallas_call(
            main_kernel,
            out_shape=[shape((3, 512, width), BF16)] * 2 + [block] * 2,
            in_specs=[VMEM] * 11, out_specs=[VMEM] * 4,
            scratch_shapes=[
                pltpu.VMEM((16 * n_tok, width), BF16), pltpu.VMEM((16 * n_tok, width), BF16),
                pltpu.VMEM((16, 64, 128), F32), pltpu.VMEM((128, width), BF16), pltpu.VMEM((128, width), BF16),
                dma((3, 4, 16)), dma((3, 16)), dma((2, 4)), dma((2, 4)),
            ],
            compiler_params=pltpu.CompilerParams(collective_id=1, has_side_effects=True, vmem_limit_bytes=32 * MB),
        )(tok, dy, g_own, xd, dyd, xu, dyu, xy, dyy, ru, rv)
        du, dv, y, dx = pl.pallas_call(
            put_kernel,
            out_shape=[table, table, block, block],
            in_specs=[VMEM] * 4 + [SMEM, VMEM, HBM, HBM], out_specs=[HBM, HBM, VMEM, VMEM],
            scratch_shapes=[pltpu.VMEM((4096, width), BF16), pltpu.VMEM((4096, width), BF16), dma((2,))],
            input_output_aliases={6: 0, 7: 1},
            compiler_params=pltpu.CompilerParams(vmem_limit_bytes=36 * MB),
        )(pu, pv, y, dx, vslot, meta, du, dv)
        return y, dx, du, dv

    return jax.shard_map(device_step, mesh=mesh, in_specs=(tok_spec, tok_spec, row_spec, row_spec, tok_spec, tok_spec, tok_spec), out_specs=(tok_spec, tok_spec, row_spec, row_spec), check_vma=False)
```

```python
import functools

import jax
import jax.numpy as jnp
from jax import lax
from jax.experimental import pallas as pl
from jax.experimental.pallas import tpu as pltpu
from jax.sharding import PartitionSpec as P

MESH = pl.DeviceIdType.MESH
F32 = jnp.float32
BF16 = jnp.bfloat16
VMEM = pl.BlockSpec(memory_space=pltpu.VMEM)
ANY = pl.BlockSpec(memory_space=pl.ANY)
NT = (((1,), (1,)), ((), ()))
TN = (((0,), (0,)), ((), ()))
HBM = pl.BlockSpec(memory_space=pltpu.HBM)
SMEM = pl.BlockSpec(memory_space=pltpu.SMEM)
MB = 1024 * 1024
UP, DOWN, YY, CC = range(4)


def gelu_pair(pre_act):
    cdf_val = 0.5 * (1.0 + lax.erf(pre_act * 0.7071067811865476))
    pdf_val = jnp.exp(-0.5 * pre_act * pre_act) * 0.3989422804014327
    return pre_act * cdf_val, cdf_val + pre_act * pdf_val


def split3(val):
    one = val.astype(BF16)
    rest = val - one.astype(F32)
    two = rest.astype(BF16)
    three = (rest - two.astype(F32)).astype(BF16)
    return one, two, three


def dot(a, b, dims=None):
    if dims is None:
        return jnp.dot(a, b, preferred_element_type=F32)
    return lax.dot_general(a, b, dims, preferred_element_type=F32)


def first_kernel(ids_ref, x_ref, dy_ref, ids_out, xd, dyd, xu, dyu, xy, dyy, ssem, rsem, hops, hopr):
    z = lax.axis_index("data")
    t = lax.axis_index("table")
    me = z * 4 + t
    bar = pltpu.get_barrier_semaphore()
    peers = [(lax.rem(z + dz, 4), lax.rem(t + dt, 4)) for dz in range(4) for dt in range(4)][1:]
    for pz, pt in peers:
        pl.semaphore_signal(bar, inc=1, device_id={"data": pz, "table": pt}, device_id_type=MESH)
    pl.semaphore_wait(bar, 15)
    copies = []
    for i, (pz, pt) in enumerate(peers):
        copies.append(pltpu.make_async_remote_copy(
            src_ref=ids_ref, dst_ref=ids_out.at[me], send_sem=ssem.at[i], recv_sem=rsem.at[i],
            device_id={"data": pz, "table": pt}, device_id_type=MESH,
        ))
        copies[-1].start()

    def hop(k, lane):
        dst = ((xd, dyd), (xu, dyu), (xy, dyy))[lane][k]
        peer = ({"data": z + 1}, {"data": z - 1}, {"table": lax.rem(t + 2, 4)})[lane]
        return pltpu.make_async_remote_copy(
            src_ref=(x_ref, dy_ref)[k], dst_ref=dst, send_sem=hops.at[k, lane], recv_sem=hopr.at[k, lane],
            device_id=peer, device_id_type=MESH,
        )

    for k in range(2):
        hop(k, 2).start()

        @pl.when(z < 3)
        def _():
            hop(k, 0).start()

        @pl.when(z > 0)
        def _():
            hop(k, 1).start()

    local = pltpu.make_async_copy(ids_ref, ids_out.at[me], ssem.at[15])
    local.start()
    local.wait()
    for one in copies:
        one.wait()
    for k in range(2):
        hop(k, 2).wait()

        @pl.when(z < 3)
        def _():
            hop(k, 0).wait_send()
            hop(k, 1).wait_recv()

        @pl.when(z > 0)
        def _():
            hop(k, 1).wait_send()
            hop(k, 0).wait_recv()


def prep_kernel(u_hbm, v_hbm, pick_hbm, gate_hbm, ids_ref, du_hbm, g_out, rows_u, rows_v, vslot, meta,
                zbuf, ugrp, vgrp, uacc, vacc, pick_ref, gate_ref, sslot, zsem, gsem, ssem, isem):
    r = lax.axis_index("table")
    n_local = u_hbm.shape[0]
    n_ent = rows_u.shape[0]
    zrows = zbuf.shape[0]
    load_pick = pltpu.make_async_copy(pick_hbm, pick_ref, isem.at[0])
    load_gate = pltpu.make_async_copy(gate_hbm, gate_ref, isem.at[1])
    load_pick.start()
    load_gate.start()
    zbuf[...] = jnp.zeros_like(zbuf)

    ids = jnp.concatenate([ids_ref[e] for e in range(16)], axis=0).astype(F32)
    pick = ids[:, 0:32]
    for o in range(1, 4):
        pick = jnp.where(r == o, ids[:, o * 32 : o * 32 + 32], pick)
    pick = pick - (r * n_local).astype(F32)
    idrow = jnp.concatenate([pick[e : e + 1, :] for e in range(16)], axis=1)
    ii = lax.broadcasted_iota(jnp.int32, (n_ent, n_ent), 0)
    jj = lax.broadcasted_iota(jnp.int32, (n_ent, n_ent), 1)

    def fill(i):
        return pltpu.make_async_copy(zbuf, du_hbm.at[pl.ds(i * zrows, zrows), :], zsem)

    for i in range(n_local // zrows):
        fill(i).start()

    def lanes(cond, val):
        return jnp.sum(jnp.where(cond, val, 0.0), axis=1, keepdims=True)

    def subl(cond, val):
        return jnp.sum(jnp.where(cond, val, 0.0), axis=0, keepdims=True)

    idcol = lanes(ii == jj, jnp.broadcast_to(idrow, (n_ent, n_ent)))
    grow, gcol = jnp.floor(idrow * 0.125), jnp.floor(idcol * 0.125)
    same = gcol == grow
    lead_col = jnp.where(lanes(same & (jj < ii), 1.0) == 0.0, 1.0, 0.0)
    lead_row = jnp.where(subl(same & (ii < jj), 1.0) == 0.0, 1.0, 0.0)
    rank_col = lanes(jj < ii, jnp.broadcast_to(lead_row, (n_ent, n_ent)))
    rank_row = subl(ii < jj, jnp.broadcast_to(lead_col, (n_ent, n_ent)))
    hit_c = (rank_col.astype(jnp.int32) == jj) & (lead_col > 0.0)
    hit_r = (rank_row.astype(jnp.int32) == ii) & (lead_row > 0.0)
    icount = jnp.sum(lead_row, axis=1, keepdims=True).astype(jnp.int32)
    slot_row = subl(hit_c, jnp.broadcast_to(gcol, (n_ent, n_ent)))
    slot_col = lanes(hit_r, jnp.broadcast_to(grow, (n_ent, n_ent)))
    vslot[0:1, :] = slot_row.astype(jnp.int32)
    vslot[1:8, :] = jnp.broadcast_to(icount, (7, n_ent))
    slot_row = jnp.where(jj[0:1, :] < icount, slot_row, -1.0)
    slot_col = jnp.where(ii[:, 0:1] < icount, slot_col, -1.0)
    meta[0:1, :] = idrow
    meta[1:8, :] = jnp.broadcast_to(slot_row, (7, n_ent))

    to_smem = pltpu.make_async_copy(vslot, sslot, ssem)
    to_smem.start()
    to_smem.wait()
    n_blk = (sslot[1, 0] + 31) // 32

    def fetch(k, table, grp, s):
        g = pl.multiple_of(sslot[0, k] * 8, 8)
        return pltpu.make_async_copy(table.at[pl.ds(g, 8), :], grp.at[pl.ds(pl.multiple_of(k * 8, 8), 8), :], gsem.at[s])

    def start_fetch(k, carry):
        fetch(k, u_hbm, ugrp, 0).start()
        fetch(k, v_hbm, vgrp, 1).start()
        return carry

    def wait_fetch(k, carry):
        fetch(k, u_hbm, ugrp, 0).wait()
        fetch(k, v_hbm, vgrp, 1).wait()
        return carry

    lax.fori_loop(0, n_blk * 32, start_fetch, 0)

    load_pick.wait()
    load_gate.wait()
    sel, tok = pick_ref.shape
    quarter = sel // 4
    row = lax.broadcasted_iota(jnp.int32, (2 * quarter, 2 * tok), 0)
    row = row + jnp.where(row >= quarter, quarter, 0)

    def add_gates(i, acc):
        base = pl.multiple_of(i * 8, 8)
        pick8 = pick_ref[pl.ds(base, 8), :]
        gate8 = gate_ref[pl.ds(base, 8), :]
        pick8 = jnp.concatenate([pick8, pick8 - quarter], axis=1)
        gate8 = jnp.concatenate([gate8, gate8], axis=1)
        for j in range(8):
            acc = acc + jnp.where(row == pick8[j : j + 1, :], gate8[j : j + 1, :], 0.0)
        return acc

    g_out[...] = lax.fori_loop(0, sel // 8, add_gates, jnp.zeros((2 * quarter, 2 * tok), F32))

    lax.fori_loop(0, n_blk * 32, wait_fetch, 0)

    uacc[...] = jnp.zeros_like(uacc)
    vacc[...] = jnp.zeros_like(vacc)
    kk = lax.broadcasted_iota(jnp.int32, (n_ent, 256), 0)
    qk = lax.broadcasted_iota(jnp.int32, (n_ent, 256), 1) >> 3
    q7 = (lax.broadcasted_iota(jnp.int32, (1, 256), 1) & 7).astype(F32)

    def take_rows(b, carry):
        rowid = 8.0 * subl(kk == qk + b * 32, jnp.broadcast_to(slot_col, (n_ent, 256))) + q7
        pickm = jnp.where(idcol == rowid, 1.0, 0.0).astype(BF16)
        base = pl.multiple_of(b * 256, 256)
        uacc[...] += dot(pickm, ugrp[pl.ds(base, 256), :])
        vacc[...] += dot(pickm, vgrp[pl.ds(base, 256), :])
        return carry

    lax.fori_loop(0, n_blk, take_rows, 0)
    rows_u[...] = uacc[...].astype(BF16)
    rows_v[...] = vacc[...].astype(BF16)
    for i in range(n_local // zrows):
        fill(i).wait()


def main_kernel(x_ref, dy_ref, g_ref, xd, dyd, xu, dyu, xy, dyy, ru, rv, pu, pv, y_out, dx_out,
                tx, ty, gx, ubuf, vbuf, ssem, rsem, rows_s, rows_r):
    z = lax.axis_index("data")
    t = lax.axis_index("table")
    y, c = t // 2, lax.rem(t, 2)
    t_y = (1 - y) * 2 + c
    t_c = y * 2 + (1 - c)
    t_yc = (1 - y) * 2 + (1 - c)
    y_peer, c_peer = {"table": t_y}, {"table": t_c}
    up, down = {"data": z + 1}, {"data": z - 1}
    peers = {UP: up, DOWN: down, YY: y_peer, CC: c_peer}
    tok = x_ref.shape[0]
    low_at = {d: z - d >= 0 for d in (1, 2, 3)}
    high_at = {d: z + d <= 3 for d in (1, 2, 3)}
    can_up, can_down = high_at[1], low_at[1]
    middle = can_up & can_down
    ends = (z == 0) | (z == 3)

    bar = pltpu.get_barrier_semaphore()
    for peer in (t_y, t_c, t_yc):
        pl.semaphore_signal(bar, inc=1, device_id={"table": peer}, device_id_type=MESH)

    @pl.when(can_up)
    def _():
        pl.semaphore_signal(bar, inc=1, device_id=up, device_id_type=MESH)

    @pl.when(can_down)
    def _():
        pl.semaphore_signal(bar, inc=1, device_id=down, device_id_type=MESH)

    pl.semaphore_wait(bar, 3 + can_up.astype(jnp.int32) + can_down.astype(jnp.int32))

    outs = (gx, tx, ty)
    TOKS = (1, 2)
    sent = []

    def place(k, slot):
        if k == 0:
            return gx.at[slot]
        return outs[k].at[pl.ds(pl.multiple_of(slot * tok, tok), tok), :]

    def copy(k, slot, lane, src=None):
        ref = place(k, slot)
        return pltpu.make_async_remote_copy(
            src_ref=ref if src is None else src, dst_ref=ref,
            send_sem=ssem.at[k, lane, slot], recv_sem=rsem.at[k, slot],
            device_id=peers[lane], device_id_type=MESH,
        )

    def when(cond, run):
        if cond is None:
            run()
        else:
            @pl.when(cond)
            def _():
                run()

    def start(cond, k, slot, lane, src=None):
        sent.append((cond, k, slot, lane))
        when(cond, lambda: copy(k, slot, lane, src).start())

    def arrive(cond, k, slot):
        when(cond, lambda: copy(k, slot, CC).wait_recv())

    def zs(d):
        return (z + d) * 4 + t

    def ys(d):
        return (z + d) * 4 + t_y

    def send_row(k, s):
        to = lax.rem(t + s, 4)
        return pltpu.make_async_remote_copy(
            src_ref=(ru, rv)[k].at[pl.ds(pl.multiple_of(z * 128 + to * 32, 32), 32), :],
            dst_ref=(ubuf, vbuf)[k].at[pl.ds(pl.multiple_of(t * 32, 32), 32), :],
            send_sem=rows_s.at[k, s], recv_sem=rows_r.at[k, s],
            device_id={"table": to}, device_id_type=MESH,
        )

    own = (None, x_ref, dy_ref)
    low = (None, xd, dyd)
    high = (None, xu, dyu)
    across = (None, xy, dyy)
    me = zs(0)
    my_half = g_ref.at[pl.ds(pl.multiple_of(y * 32, 32), 32), :]
    other_half = g_ref.at[pl.ds(pl.multiple_of((1 - y) * 32, 32), 32), :]

    start(can_up, 0, me, UP, my_half)
    start(can_down, 0, me, DOWN, my_half)
    start(None, 0, me, YY, other_half)
    start(None, 0, me, CC, my_half)
    for k in TOKS:
        start(middle, k, zs(-1), UP, low[k])
        start(middle, k, zs(1), DOWN, high[k])
    for k in range(2):
        for s in (2, 1, 3):
            send_row(k, s).start()
    for k in TOKS:
        start(z < 2, k, ys(0), UP, across[k])
        start(z > 1, k, ys(0), DOWN, across[k])
        start(None, k, me, CC, own[k])
        start(None, k, ys(0), CC, across[k])
        start(can_down, k, zs(-1), CC, low[k])
        start(can_up, k, zs(1), CC, high[k])

    def keep(cond, k, slot, src):
        def run():
            outs[k][pl.ds(pl.multiple_of(slot * tok, tok), tok), :] = src[...]

        when(cond, run)

    gx[me] = g_ref[pl.ds(pl.multiple_of(y * 32, 32), 32), :]
    for k in TOKS:
        keep(None, k, me, own[k])
        keep(None, k, ys(0), across[k])
        keep(can_down, k, zs(-1), low[k])
        keep(can_up, k, zs(1), high[k])
    mine = pl.ds(pl.multiple_of(t * 32, 32), 32)
    ubuf[mine, :] = ru[pl.ds(pl.multiple_of(z * 128 + t * 32, 32), 32), :]
    vbuf[mine, :] = rv[pl.ds(pl.multiple_of(z * 128 + t * 32, 32), 32), :]

    def gates_on(slot_of, d):
        arrive(low_at[d], 0, slot_of(-d))
        start(low_at[d] & can_up, 0, slot_of(-d), UP)
        start(low_at[d], 0, slot_of(-d), CC)
        arrive(high_at[d], 0, slot_of(d))
        start(high_at[d] & can_down, 0, slot_of(d), DOWN)
        start(high_at[d], 0, slot_of(d), CC)

    def tokens_on(d):
        for k in TOKS:
            arrive(low_at[d], k, zs(-d))
            start(low_at[d] & can_up, k, zs(-d), UP)
            start(low_at[d], k, zs(-d), YY)
            arrive(high_at[d], k, zs(d))
            start(high_at[d] & can_down, k, zs(d), DOWN)
            start(high_at[d], k, zs(d), YY)
            start(low_at[d], k, zs(-d), CC)
            start(high_at[d], k, zs(d), CC)

    def crossed(cond, d):
        for k in TOKS:
            arrive(cond, k, ys(d))
            start(cond, k, ys(d), CC)

    diag = (lax.broadcasted_iota(jnp.int32, (128, 256), 0) >> 5) == (lax.broadcasted_iota(jnp.int32, (128, 256), 1) >> 6)

    def products(d):
        for tt in (t_c, t_yc):
            for k in range(3):
                arrive(None, k, d * 4 + tt)
        tsl = pl.ds(pl.multiple_of(d * 256, 256), 256)
        esl = pl.ds(pl.multiple_of(d * 128, 128), 128)
        x4, dy4 = tx[tsl, :], ty[tsl, :]
        u4, v4 = ru[esl, :], rv[esl, :]
        gates = []
        for e in range(4):
            part = gx[d * 4 + e]
            part = jnp.where(c == 1, part[:, 64:128], part[:, 0:64])
            gates.append(jnp.concatenate([part] * 4, axis=1))
        g4 = jnp.concatenate(gates, axis=0)
        act, slope = gelu_pair(dot(u4, x4, NT))
        b4 = dot(v4, dy4, NT)
        w4 = jnp.where(diag, g4 * act, 0.0)
        c4 = jnp.where(diag, g4 * slope * b4, 0.0)
        for coef, val, out in ((c4, x4, pu), (w4, dy4, pv)):
            full = dot(jnp.concatenate(split3(coef), axis=0), val)
            full = full[0:128] + full[128:256] + full[256:384]
            for k, term in enumerate(split3(full)):
                out[k, esl, :] = term

    gates_on(zs, 1)
    arrive(None, 0, ys(0))
    start(can_up, 0, ys(0), UP)
    start(can_down, 0, ys(0), DOWN)
    start(None, 0, ys(0), CC)
    gates_on(zs, 2)
    gates_on(ys, 1)
    products(z)
    tokens_on(2)
    for k in TOKS:
        start(z == 2, k, ys(0), UP, across[k])
        start(z == 1, k, ys(0), DOWN, across[k])
    gates_on(zs, 3)
    gates_on(ys, 2)
    gates_on(ys, 3)

    gates = jnp.concatenate([g_ref[0:32, 0:64], g_ref[0:32, 64:128], g_ref[32:64, 0:64], g_ref[32:64, 64:128]], axis=0)
    for s in range(1, 4):
        send_row(0, s).wait_recv()
        send_row(1, s).wait_recv()
    act, slope = gelu_pair(dot(ubuf[...], x_ref[...], NT))
    b_val = dot(vbuf[...], dy_ref[...], NT)
    w_val = jnp.transpose(gates * act)
    c_val = jnp.transpose(gates * slope * b_val)
    for coef, rows, out in ((w_val, vbuf, y_out), (c_val, ubuf, dx_out)):
        full = dot(jnp.concatenate(split3(coef), axis=0), rows[...])
        out[...] = (full[0:64] + full[64:128] + full[128:192]).astype(BF16)

    tokens_on(3)
    crossed(middle, -1)
    crossed(middle, 1)
    when(middle, lambda: products(z - 1))
    when(middle, lambda: products(z + 1))
    crossed(low_at[2], -2)
    crossed(high_at[2], 2)
    products(lax.rem(z + 2, 4))
    crossed(z == 3, -1)
    crossed(z == 0, 1)
    when(ends, lambda: products(1 + z // 3))
    crossed(low_at[3], -3)
    crossed(high_at[3], 3)
    when(ends, lambda: products(3 - z))

    for k in range(2):
        for s in range(1, 4):
            send_row(k, s).wait_send()
    for cond, k, slot, lane in sent:
        when(cond, lambda k=k, slot=slot, lane=lane: copy(k, slot, lane).wait_send())


def put_kernel(pu, pv, y_ref, dx_ref, sslot, meta, du_in, du_hbm, dv_hbm, y_out, dx_out, zbuf, ures, vres, zsem, psem):
    n_ent = pu.shape[1]
    zrows = zbuf.shape[0]
    zbuf[...] = jnp.zeros_like(zbuf)
    y_out[...] = y_ref[...]
    dx_out[...] = dx_ref[...]
    n_slot = sslot[1, 0]
    n_blk = (n_slot + 31) // 32
    idrow, slot_row = meta[0:1, :], meta[1:2, :]
    kq = lax.broadcasted_iota(jnp.int32, (256, n_ent), 1)
    qq = lax.broadcasted_iota(jnp.int32, (256, n_ent), 0) >> 3
    q7 = (lax.broadcasted_iota(jnp.int32, (256, 1), 0) & 7).astype(F32)

    def fill(i):
        return pltpu.make_async_copy(zbuf, dv_hbm.at[pl.ds(i * zrows, zrows), :], zsem)

    for i in range(dv_hbm.shape[0] // zrows):
        fill(i).start()

    def patch(k, table, res, s):
        g = pl.multiple_of(sslot[0, k] * 8, 8)
        return pltpu.make_async_copy(res.at[pl.ds(pl.multiple_of(k * 8, 8), 8), :], table.at[pl.ds(g, 8), :], psem.at[s])

    def put_rows(b, carry):
        rowid = 8.0 * jnp.sum(jnp.where(kq == qq + b * 32, slot_row, 0.0), axis=1, keepdims=True) + q7
        spread = jnp.where(rowid == idrow, 1.0, 0.0).astype(BF16)
        base = pl.multiple_of(b * 256, 256)
        ures[pl.ds(base, 256), :] = (dot(spread, pu[0]) + dot(spread, pu[1]) + dot(spread, pu[2])).astype(BF16)
        vres[pl.ds(base, 256), :] = (dot(spread, pv[0]) + dot(spread, pv[1]) + dot(spread, pv[2])).astype(BF16)
        return carry

    lax.fori_loop(0, n_blk, put_rows, 0)

    def over_slots(run):
        def body(k, carry):
            run(k)
            return carry

        lax.fori_loop(0, n_slot, body, 0)

    over_slots(lambda k: patch(k, du_hbm, ures, 0).start())
    for i in range(dv_hbm.shape[0] // zrows):
        fill(i).wait()
    over_slots(lambda k: patch(k, dv_hbm, vres, 1).start())
    over_slots(lambda k: patch(k, du_hbm, ures, 0).wait())
    over_slots(lambda k: patch(k, dv_hbm, vres, 1).wait())


def solution(mesh):
    tok_spec = P(('replica', 'data', 'table'))
    row_spec = P(('replica', 'table'))

    def device_step(tok, dy, u, v, wanted, pick, gate):
        n_tok, width = tok.shape
        n_local = u.shape[0]
        sel = pick.shape[1] * pick.shape[2]
        shape = jax.ShapeDtypeStruct
        dma = pltpu.SemaphoreType.DMA
        rows = shape((512, width), BF16)
        block = shape((n_tok, width), BF16)
        table = shape((n_local, width), BF16)
        pick_t = jnp.transpose(pick, (1, 2, 0)).reshape(sel, n_tok)
        gate_t = jnp.transpose(gate, (1, 2, 0)).reshape(sel, n_tok)

        ids, *hops = pl.pallas_call(
            first_kernel, out_shape=[shape((16, 1, 128), jnp.int32)] + [block] * 6,
            in_specs=[HBM] * 3, out_specs=[VMEM] * 7,
            scratch_shapes=[dma((16,)), dma((15,)), dma((2, 3)), dma((2, 3))],
            compiler_params=pltpu.CompilerParams(collective_id=0, has_side_effects=True, vmem_limit_bytes=4 * MB),
        )(wanted, tok, dy)
        du, g_own, ru, rv, vslot, meta = pl.pallas_call(
            prep_kernel,
            out_shape=[table, shape((64, 128), F32), rows, rows, shape((8, 512), jnp.int32), shape((8, 512), F32)],
            in_specs=[HBM] * 4 + [VMEM], out_specs=[HBM] + [VMEM] * 5,
            scratch_shapes=[
                pltpu.VMEM((512, width), BF16), pltpu.VMEM((4096, width), BF16), pltpu.VMEM((4096, width), BF16),
                pltpu.VMEM((512, width), F32), pltpu.VMEM((512, width), F32),
                pltpu.VMEM((sel, n_tok), jnp.int32), pltpu.VMEM((sel, n_tok), F32),
                pltpu.SMEM((8, 512), jnp.int32), dma, dma((2,)), dma, dma((2,)),
            ],
            compiler_params=pltpu.CompilerParams(vmem_limit_bytes=36 * MB),
        )(u, v, pick_t, gate_t, ids)
        pu, pv, y, dx = pl.pallas_call(
            main_kernel,
            out_shape=[shape((3, 512, width), BF16)] * 2 + [block] * 2,
            in_specs=[VMEM] * 11, out_specs=[VMEM] * 4,
            scratch_shapes=[
                pltpu.VMEM((16 * n_tok, width), BF16), pltpu.VMEM((16 * n_tok, width), BF16),
                pltpu.VMEM((16, 32, 128), F32), pltpu.VMEM((128, width), BF16), pltpu.VMEM((128, width), BF16),
                dma((3, 4, 16)), dma((3, 16)), dma((2, 4)), dma((2, 4)),
            ],
            compiler_params=pltpu.CompilerParams(collective_id=1, has_side_effects=True, vmem_limit_bytes=32 * MB),
        )(tok, dy, g_own, *hops, ru, rv)
        du, dv, y, dx = pl.pallas_call(
            put_kernel,
            out_shape=[table, table, block, block],
            in_specs=[VMEM] * 4 + [SMEM, VMEM, HBM], out_specs=[HBM, HBM, VMEM, VMEM],
            scratch_shapes=[
                pltpu.VMEM((512, width), BF16), pltpu.VMEM((4096, width), BF16), pltpu.VMEM((4096, width), BF16),
                dma, dma((2,)),
            ],
            input_output_aliases={6: 0},
            compiler_params=pltpu.CompilerParams(vmem_limit_bytes=36 * MB),
        )(pu, pv, y, dx, vslot, meta, du)
        return y, dx, du, dv

    return jax.shard_map(device_step, mesh=mesh, in_specs=(tok_spec, tok_spec, row_spec, row_spec, tok_spec, tok_spec, tok_spec), out_specs=(tok_spec, tok_spec, row_spec, row_spec), check_vma=False)
```

```python
import functools

import jax
import jax.numpy as jnp
from jax import lax
from jax.experimental import pallas as pl
from jax.experimental.pallas import tpu as pltpu
from jax.sharding import PartitionSpec as P

MESH = pl.DeviceIdType.MESH
F32 = jnp.float32
BF16 = jnp.bfloat16
VMEM = pl.BlockSpec(memory_space=pltpu.VMEM)
ANY = pl.BlockSpec(memory_space=pl.ANY)
NT = (((1,), (1,)), ((), ()))
TN = (((0,), (0,)), ((), ()))
HBM = pl.BlockSpec(memory_space=pltpu.HBM)
SMEM = pl.BlockSpec(memory_space=pltpu.SMEM)
MB = 1024 * 1024
UP, DOWN, YY, CC = range(4)


def gelu_pair(pre_act):
    cdf_val = 0.5 * (1.0 + lax.erf(pre_act * 0.7071067811865476))
    pdf_val = jnp.exp(-0.5 * pre_act * pre_act) * 0.3989422804014327
    return pre_act * cdf_val, cdf_val + pre_act * pdf_val


def split3(val):
    one = val.astype(BF16)
    rest = val - one.astype(F32)
    two = rest.astype(BF16)
    three = (rest - two.astype(F32)).astype(BF16)
    return one, two, three


def dot(a, b, dims=None):
    if dims is None:
        return jnp.dot(a, b, preferred_element_type=F32)
    return lax.dot_general(a, b, dims, preferred_element_type=F32)


def first_kernel(ids_ref, x_ref, dy_ref, ids_out, xd, dyd, xu, dyu, xy, dyy, ssem, rsem, hops, hopr):
    z = lax.axis_index("data")
    t = lax.axis_index("table")
    me = z * 4 + t
    bar = pltpu.get_barrier_semaphore()
    peers = [(lax.rem(z + dz, 4), lax.rem(t + dt, 4)) for dz in range(4) for dt in range(4)][1:]
    for pz, pt in peers:
        pl.semaphore_signal(bar, inc=1, device_id={"data": pz, "table": pt}, device_id_type=MESH)
    pl.semaphore_wait(bar, 15)
    copies = []
    for i, (pz, pt) in enumerate(peers):
        copies.append(pltpu.make_async_remote_copy(
            src_ref=ids_ref, dst_ref=ids_out.at[me], send_sem=ssem.at[i], recv_sem=rsem.at[i],
            device_id={"data": pz, "table": pt}, device_id_type=MESH,
        ))
        copies[-1].start()

    def hop(k, lane):
        dst = ((xd, dyd), (xu, dyu), (xy, dyy))[lane][k]
        peer = ({"data": z + 1}, {"data": z - 1}, {"table": lax.rem(t + 2, 4)})[lane]
        return pltpu.make_async_remote_copy(
            src_ref=(x_ref, dy_ref)[k], dst_ref=dst, send_sem=hops.at[k, lane], recv_sem=hopr.at[k, lane],
            device_id=peer, device_id_type=MESH,
        )

    for k in range(2):
        hop(k, 2).start()

        @pl.when(z < 3)
        def _():
            hop(k, 0).start()

        @pl.when(z > 0)
        def _():
            hop(k, 1).start()

    local = pltpu.make_async_copy(ids_ref, ids_out.at[me], ssem.at[15])
    local.start()
    local.wait()
    for one in copies:
        one.wait()
    for k in range(2):
        hop(k, 2).wait()

        @pl.when(z < 3)
        def _():
            hop(k, 0).wait_send()
            hop(k, 1).wait_recv()

        @pl.when(z > 0)
        def _():
            hop(k, 1).wait_send()
            hop(k, 0).wait_recv()


def prep_kernel(u_hbm, v_hbm, pick_hbm, gate_hbm, ids_ref, du_hbm, g_out, rows_u, rows_v, vslot, meta,
                zbuf, ugrp, vgrp, uacc, vacc, pick_ref, gate_ref, sslot, zsem, gsem, ssem, isem):
    r = lax.axis_index("table")
    n_local = u_hbm.shape[0]
    n_ent = rows_u.shape[0]
    zrows = zbuf.shape[0]
    load_pick = pltpu.make_async_copy(pick_hbm, pick_ref, isem.at[0])
    load_gate = pltpu.make_async_copy(gate_hbm, gate_ref, isem.at[1])
    load_pick.start()
    load_gate.start()
    zbuf[...] = jnp.zeros_like(zbuf)

    ids = jnp.concatenate([ids_ref[e] for e in range(16)], axis=0).astype(F32)
    pick = ids[:, 0:32]
    for o in range(1, 4):
        pick = jnp.where(r == o, ids[:, o * 32 : o * 32 + 32], pick)
    pick = pick - (r * n_local).astype(F32)
    idrow = jnp.concatenate([pick[e : e + 1, :] for e in range(16)], axis=1)
    ii = lax.broadcasted_iota(jnp.int32, (n_ent, n_ent), 0)
    jj = lax.broadcasted_iota(jnp.int32, (n_ent, n_ent), 1)

    def fill(i):
        return pltpu.make_async_copy(zbuf, du_hbm.at[pl.ds(i * zrows, zrows), :], zsem)

    for i in range(n_local // zrows):
        fill(i).start()

    def lanes(cond, val):
        return jnp.sum(jnp.where(cond, val, 0.0), axis=1, keepdims=True)

    def subl(cond, val):
        return jnp.sum(jnp.where(cond, val, 0.0), axis=0, keepdims=True)

    idcol = lanes(ii == jj, jnp.broadcast_to(idrow, (n_ent, n_ent)))
    grow, gcol = jnp.floor(idrow * 0.125), jnp.floor(idcol * 0.125)
    same = gcol == grow
    lead_col = jnp.where(lanes(same & (jj < ii), 1.0) == 0.0, 1.0, 0.0)
    lead_row = jnp.where(subl(same & (ii < jj), 1.0) == 0.0, 1.0, 0.0)
    rank_col = lanes(jj < ii, jnp.broadcast_to(lead_row, (n_ent, n_ent)))
    rank_row = subl(ii < jj, jnp.broadcast_to(lead_col, (n_ent, n_ent)))
    hit_c = (rank_col.astype(jnp.int32) == jj) & (lead_col > 0.0)
    hit_r = (rank_row.astype(jnp.int32) == ii) & (lead_row > 0.0)
    icount = jnp.sum(lead_row, axis=1, keepdims=True).astype(jnp.int32)
    slot_row = subl(hit_c, jnp.broadcast_to(gcol, (n_ent, n_ent)))
    slot_col = lanes(hit_r, jnp.broadcast_to(grow, (n_ent, n_ent)))
    vslot[0:1, :] = slot_row.astype(jnp.int32)
    vslot[1:8, :] = jnp.broadcast_to(icount, (7, n_ent))
    slot_row = jnp.where(jj[0:1, :] < icount, slot_row, -1.0)
    slot_col = jnp.where(ii[:, 0:1] < icount, slot_col, -1.0)
    meta[0:1, :] = idrow
    meta[1:8, :] = jnp.broadcast_to(slot_row, (7, n_ent))

    to_smem = pltpu.make_async_copy(vslot, sslot, ssem)
    to_smem.start()
    to_smem.wait()
    n_blk = (sslot[1, 0] + 31) // 32

    def fetch(k, table, grp, s):
        g = pl.multiple_of(sslot[0, k] * 8, 8)
        return pltpu.make_async_copy(table.at[pl.ds(g, 8), :], grp.at[pl.ds(pl.multiple_of(k * 8, 8), 8), :], gsem.at[s])

    def start_fetch(k, carry):
        fetch(k, u_hbm, ugrp, 0).start()
        fetch(k, v_hbm, vgrp, 1).start()
        return carry

    def wait_fetch(k, carry):
        fetch(k, u_hbm, ugrp, 0).wait()
        fetch(k, v_hbm, vgrp, 1).wait()
        return carry

    lax.fori_loop(0, n_blk * 32, start_fetch, 0)

    load_pick.wait()
    load_gate.wait()
    sel, tok = pick_ref.shape
    quarter = sel // 4
    row = lax.broadcasted_iota(jnp.int32, (2 * quarter, 2 * tok), 0)
    row = row + jnp.where(row >= quarter, quarter, 0)

    def add_gates(i, acc):
        base = pl.multiple_of(i * 8, 8)
        pick8 = pick_ref[pl.ds(base, 8), :]
        gate8 = gate_ref[pl.ds(base, 8), :]
        pick8 = jnp.concatenate([pick8, pick8 - quarter], axis=1)
        gate8 = jnp.concatenate([gate8, gate8], axis=1)
        for j in range(8):
            acc = acc + jnp.where(row == pick8[j : j + 1, :], gate8[j : j + 1, :], 0.0)
        return acc

    g_out[...] = lax.fori_loop(0, sel // 8, add_gates, jnp.zeros((2 * quarter, 2 * tok), F32))

    lax.fori_loop(0, n_blk * 32, wait_fetch, 0)

    uacc[...] = jnp.zeros_like(uacc)
    vacc[...] = jnp.zeros_like(vacc)
    kk = lax.broadcasted_iota(jnp.int32, (n_ent, 256), 0)
    qk = lax.broadcasted_iota(jnp.int32, (n_ent, 256), 1) >> 3
    q7 = (lax.broadcasted_iota(jnp.int32, (1, 256), 1) & 7).astype(F32)

    def take_rows(b, carry):
        rowid = 8.0 * subl(kk == qk + b * 32, jnp.broadcast_to(slot_col, (n_ent, 256))) + q7
        pickm = jnp.where(idcol == rowid, 1.0, 0.0).astype(BF16)
        base = pl.multiple_of(b * 256, 256)
        uacc[...] += dot(pickm, ugrp[pl.ds(base, 256), :])
        vacc[...] += dot(pickm, vgrp[pl.ds(base, 256), :])
        return carry

    lax.fori_loop(0, n_blk, take_rows, 0)
    rows_u[...] = uacc[...].astype(BF16)
    rows_v[...] = vacc[...].astype(BF16)
    for i in range(n_local // zrows):
        fill(i).wait()


def main_kernel(x_ref, dy_ref, g_ref, xd, dyd, xu, dyu, xy, dyy, ru, rv, pu, pv, y_out, dx_out,
                tx, ty, gx, ubuf, vbuf, ssem, rsem, rows_s, rows_r):
    z = lax.axis_index("data")
    t = lax.axis_index("table")
    y, c = t // 2, lax.rem(t, 2)
    t_y = (1 - y) * 2 + c
    t_c = y * 2 + (1 - c)
    t_yc = (1 - y) * 2 + (1 - c)
    y_peer, c_peer = {"table": t_y}, {"table": t_c}
    up, down = {"data": z + 1}, {"data": z - 1}
    peers = {UP: up, DOWN: down, YY: y_peer, CC: c_peer}
    tok = x_ref.shape[0]
    low_at = {d: z - d >= 0 for d in (1, 2, 3)}
    high_at = {d: z + d <= 3 for d in (1, 2, 3)}
    can_up, can_down = high_at[1], low_at[1]
    middle = can_up & can_down
    ends = (z == 0) | (z == 3)

    bar = pltpu.get_barrier_semaphore()
    for peer in (t_y, t_c, t_yc):
        pl.semaphore_signal(bar, inc=1, device_id={"table": peer}, device_id_type=MESH)

    @pl.when(can_up)
    def _():
        pl.semaphore_signal(bar, inc=1, device_id=up, device_id_type=MESH)

    @pl.when(can_down)
    def _():
        pl.semaphore_signal(bar, inc=1, device_id=down, device_id_type=MESH)

    pl.semaphore_wait(bar, 3 + can_up.astype(jnp.int32) + can_down.astype(jnp.int32))

    outs = (gx, tx, ty)
    TOKS = (1, 2)
    sent = []

    def place(k, slot):
        if k == 0:
            return gx.at[slot]
        return outs[k].at[pl.ds(pl.multiple_of(slot * tok, tok), tok), :]

    def copy(k, slot, lane, src=None):
        ref = place(k, slot)
        return pltpu.make_async_remote_copy(
            src_ref=ref if src is None else src, dst_ref=ref,
            send_sem=ssem.at[k, lane, slot], recv_sem=rsem.at[k, slot],
            device_id=peers[lane], device_id_type=MESH,
        )

    def when(cond, run):
        if cond is None:
            run()
        else:
            @pl.when(cond)
            def _():
                run()

    def start(cond, k, slot, lane, src=None):
        sent.append((cond, k, slot, lane))
        when(cond, lambda: copy(k, slot, lane, src).start())

    def arrive(cond, k, slot):
        when(cond, lambda: copy(k, slot, CC).wait_recv())

    def zs(d):
        return (z + d) * 4 + t

    def ys(d):
        return (z + d) * 4 + t_y

    def send_row(k, s):
        to = lax.rem(t + s, 4)
        return pltpu.make_async_remote_copy(
            src_ref=(ru, rv)[k].at[pl.ds(pl.multiple_of(z * 128 + to * 32, 32), 32), :],
            dst_ref=(ubuf, vbuf)[k].at[pl.ds(pl.multiple_of(t * 32, 32), 32), :],
            send_sem=rows_s.at[k, s], recv_sem=rows_r.at[k, s],
            device_id={"table": to}, device_id_type=MESH,
        )

    own = (None, x_ref, dy_ref)
    low = (None, xd, dyd)
    high = (None, xu, dyu)
    across = (None, xy, dyy)
    me = zs(0)
    my_half = g_ref.at[pl.ds(pl.multiple_of(y * 32, 32), 32), :]
    other_half = g_ref.at[pl.ds(pl.multiple_of((1 - y) * 32, 32), 32), :]

    start(can_up, 0, me, UP, my_half)
    start(can_down, 0, me, DOWN, my_half)
    start(None, 0, me, YY, other_half)
    start(None, 0, me, CC, my_half)
    for k in TOKS:
        start(middle, k, zs(-1), UP, low[k])
        start(middle, k, zs(1), DOWN, high[k])
    for k in range(2):
        for s in (2, 1, 3):
            send_row(k, s).start()
    for k in TOKS:
        start(None, k, me, CC, own[k])
        start(None, k, ys(0), CC, across[k])
        start(can_down, k, zs(-1), CC, low[k])
        start(can_up, k, zs(1), CC, high[k])

    def keep(cond, k, slot, src):
        def run():
            outs[k][pl.ds(pl.multiple_of(slot * tok, tok), tok), :] = src[...]

        when(cond, run)

    gx[me] = g_ref[pl.ds(pl.multiple_of(y * 32, 32), 32), :]
    for k in TOKS:
        keep(None, k, me, own[k])
        keep(None, k, ys(0), across[k])
        keep(can_down, k, zs(-1), low[k])
        keep(can_up, k, zs(1), high[k])
    mine = pl.ds(pl.multiple_of(t * 32, 32), 32)
    ubuf[mine, :] = ru[pl.ds(pl.multiple_of(z * 128 + t * 32, 32), 32), :]
    vbuf[mine, :] = rv[pl.ds(pl.multiple_of(z * 128 + t * 32, 32), 32), :]

    def gates_on(slot_of, d, from_low=None, from_high=None):
        from_low = low_at[d] if from_low is None else from_low
        from_high = high_at[d] if from_high is None else from_high
        arrive(from_low, 0, slot_of(-d))
        start(from_low & can_up, 0, slot_of(-d), UP)
        start(from_low, 0, slot_of(-d), CC)
        arrive(from_high, 0, slot_of(d))
        start(from_high & can_down, 0, slot_of(d), DOWN)
        start(from_high, 0, slot_of(d), CC)

    def tokens_on(d):
        for k in TOKS:
            arrive(low_at[d], k, zs(-d))
            start(low_at[d] & can_up, k, zs(-d), UP)
            start(low_at[d], k, zs(-d), YY)
            arrive(high_at[d], k, zs(d))
            start(high_at[d] & can_down, k, zs(d), DOWN)
            start(high_at[d], k, zs(d), YY)
            start(low_at[d], k, zs(-d), CC)
            start(high_at[d], k, zs(d), CC)

    def crossed(cond, d):
        for k in TOKS:
            arrive(cond, k, ys(d))
            start(cond, k, ys(d), CC)

    diag = (lax.broadcasted_iota(jnp.int32, (128, 256), 0) >> 5) == (lax.broadcasted_iota(jnp.int32, (128, 256), 1) >> 6)

    def products(d):
        for tt in (t_c, t_yc):
            for k in range(3):
                arrive(None, k, d * 4 + tt)
        tsl = pl.ds(pl.multiple_of(d * 256, 256), 256)
        esl = pl.ds(pl.multiple_of(d * 128, 128), 128)
        x4, dy4 = tx[tsl, :], ty[tsl, :]
        u4, v4 = ru[esl, :], rv[esl, :]
        gates = []
        for e in range(4):
            part = gx[d * 4 + e]
            part = jnp.where(c == 1, part[:, 64:128], part[:, 0:64])
            gates.append(jnp.concatenate([part] * 4, axis=1))
        g4 = jnp.concatenate(gates, axis=0)
        act, slope = gelu_pair(dot(u4, x4, NT))
        b4 = dot(v4, dy4, NT)
        w4 = jnp.where(diag, g4 * act, 0.0)
        c4 = jnp.where(diag, g4 * slope * b4, 0.0)
        for coef, val, out in ((c4, x4, pu), (w4, dy4, pv)):
            full = dot(jnp.concatenate(split3(coef), axis=0), val)
            full = full[0:128] + full[128:256] + full[256:384]
            for k, term in enumerate(split3(full)):
                out[k, esl, :] = term

    def cross_on(go_up, go_down):
        for k in (0, 1, 2):
            start(go_up, k, ys(0), UP, across[k])
            start(go_down, k, ys(0), DOWN, across[k])

    gates_on(zs, 1)
    arrive(None, 0, ys(0))
    cross_on(z < 2, z > 1)
    start(None, 0, ys(0), CC)
    products(z)
    tokens_on(2)
    gates_on(zs, 2)
    gates_on(ys, 1, middle, middle)
    cross_on(z == 2, z == 1)

    gates = jnp.concatenate([g_ref[0:32, 0:64], g_ref[0:32, 64:128], g_ref[32:64, 0:64], g_ref[32:64, 64:128]], axis=0)
    for s in range(1, 4):
        send_row(0, s).wait_recv()
        send_row(1, s).wait_recv()
    act, slope = gelu_pair(dot(ubuf[...], x_ref[...], NT))
    b_val = dot(vbuf[...], dy_ref[...], NT)
    w_val = jnp.transpose(gates * act)
    c_val = jnp.transpose(gates * slope * b_val)
    for coef, rows, out in ((w_val, vbuf, y_out), (c_val, ubuf, dx_out)):
        full = dot(jnp.concatenate(split3(coef), axis=0), rows[...])
        out[...] = (full[0:64] + full[64:128] + full[128:192]).astype(BF16)

    tokens_on(3)
    gates_on(zs, 3)
    crossed(middle, -1)
    crossed(middle, 1)
    gates_on(ys, 2)
    when(middle, lambda: products(z - 1))
    when(middle, lambda: products(z + 1))
    crossed(low_at[2], -2)
    crossed(high_at[2], 2)
    products(lax.rem(z + 2, 4))
    gates_on(ys, 1, z == 3, z == 0)
    crossed(z == 3, -1)
    crossed(z == 0, 1)
    when(ends, lambda: products(1 + z // 3))
    gates_on(ys, 3)
    crossed(low_at[3], -3)
    crossed(high_at[3], 3)
    when(ends, lambda: products(3 - z))

    for k in range(2):
        for s in range(1, 4):
            send_row(k, s).wait_send()
    for cond, k, slot, lane in sent:
        when(cond, lambda k=k, slot=slot, lane=lane: copy(k, slot, lane).wait_send())


def put_kernel(pu, pv, y_ref, dx_ref, sslot, meta, du_in, du_hbm, dv_hbm, y_out, dx_out, zbuf, ures, vres, zsem, psem):
    n_ent = pu.shape[1]
    zrows = zbuf.shape[0]
    zbuf[...] = jnp.zeros_like(zbuf)
    y_out[...] = y_ref[...]
    dx_out[...] = dx_ref[...]
    n_slot = sslot[1, 0]
    n_blk = (n_slot + 31) // 32
    idrow, slot_row = meta[0:1, :], meta[1:2, :]
    kq = lax.broadcasted_iota(jnp.int32, (256, n_ent), 1)
    qq = lax.broadcasted_iota(jnp.int32, (256, n_ent), 0) >> 3
    q7 = (lax.broadcasted_iota(jnp.int32, (256, 1), 0) & 7).astype(F32)

    def fill(i):
        return pltpu.make_async_copy(zbuf, dv_hbm.at[pl.ds(i * zrows, zrows), :], zsem)

    for i in range(dv_hbm.shape[0] // zrows):
        fill(i).start()

    def patch(k, table, res, s):
        g = pl.multiple_of(sslot[0, k] * 8, 8)
        return pltpu.make_async_copy(res.at[pl.ds(pl.multiple_of(k * 8, 8), 8), :], table.at[pl.ds(g, 8), :], psem.at[s])

    def put_rows(b, carry):
        rowid = 8.0 * jnp.sum(jnp.where(kq == qq + b * 32, slot_row, 0.0), axis=1, keepdims=True) + q7
        spread = jnp.where(rowid == idrow, 1.0, 0.0).astype(BF16)
        base = pl.multiple_of(b * 256, 256)
        ures[pl.ds(base, 256), :] = (dot(spread, pu[0]) + dot(spread, pu[1]) + dot(spread, pu[2])).astype(BF16)
        vres[pl.ds(base, 256), :] = (dot(spread, pv[0]) + dot(spread, pv[1]) + dot(spread, pv[2])).astype(BF16)
        return carry

    lax.fori_loop(0, n_blk, put_rows, 0)

    def over_slots(run):
        def body(k, carry):
            run(k)
            return carry

        lax.fori_loop(0, n_slot, body, 0)

    over_slots(lambda k: patch(k, du_hbm, ures, 0).start())
    for i in range(dv_hbm.shape[0] // zrows):
        fill(i).wait()
    over_slots(lambda k: patch(k, dv_hbm, vres, 1).start())
    over_slots(lambda k: patch(k, du_hbm, ures, 0).wait())
    over_slots(lambda k: patch(k, dv_hbm, vres, 1).wait())


def in_hbm(*vals):
    return [pltpu.with_memory_space_constraint(val, pltpu.HBM) for val in vals]


def solution(mesh):
    tok_spec = P(('replica', 'data', 'table'))
    row_spec = P(('replica', 'table'))

    def device_step(tok, dy, u, v, wanted, pick, gate):
        n_tok, width = tok.shape
        n_local = u.shape[0]
        sel = pick.shape[1] * pick.shape[2]
        shape = jax.ShapeDtypeStruct
        dma = pltpu.SemaphoreType.DMA
        rows = shape((512, width), BF16)
        block = shape((n_tok, width), BF16)
        table = shape((n_local, width), BF16)
        pick_t = jnp.transpose(pick, (1, 2, 0)).reshape(sel, n_tok)
        gate_t = jnp.transpose(gate, (1, 2, 0)).reshape(sel, n_tok)

        ids, *hops = pl.pallas_call(
            first_kernel, out_shape=[shape((16, 1, 128), jnp.int32)] + [block] * 6,
            in_specs=[HBM] * 3, out_specs=[VMEM] * 7,
            scratch_shapes=[dma((16,)), dma((15,)), dma((2, 3)), dma((2, 3))],
            compiler_params=pltpu.CompilerParams(collective_id=0, has_side_effects=True, vmem_limit_bytes=4 * MB),
        )(*in_hbm(wanted, tok, dy))
        du, g_own, ru, rv, vslot, meta = pl.pallas_call(
            prep_kernel,
            out_shape=[table, shape((64, 128), F32), rows, rows, shape((8, 512), jnp.int32), shape((8, 512), F32)],
            in_specs=[HBM] * 4 + [VMEM], out_specs=[HBM] + [VMEM] * 5,
            scratch_shapes=[
                pltpu.VMEM((512, width), BF16), pltpu.VMEM((4096, width), BF16), pltpu.VMEM((4096, width), BF16),
                pltpu.VMEM((512, width), F32), pltpu.VMEM((512, width), F32),
                pltpu.VMEM((sel, n_tok), jnp.int32), pltpu.VMEM((sel, n_tok), F32),
                pltpu.SMEM((8, 512), jnp.int32), dma, dma((2,)), dma, dma((2,)),
            ],
            compiler_params=pltpu.CompilerParams(vmem_limit_bytes=36 * MB),
        )(u, v, *in_hbm(pick_t, gate_t), ids)
        pu, pv, y, dx = pl.pallas_call(
            main_kernel,
            out_shape=[shape((3, 512, width), BF16)] * 2 + [block] * 2,
            in_specs=[VMEM] * 11, out_specs=[VMEM] * 4,
            scratch_shapes=[
                pltpu.VMEM((16 * n_tok, width), BF16), pltpu.VMEM((16 * n_tok, width), BF16),
                pltpu.VMEM((16, 32, 128), F32), pltpu.VMEM((128, width), BF16), pltpu.VMEM((128, width), BF16),
                dma((3, 4, 16)), dma((3, 16)), dma((2, 4)), dma((2, 4)),
            ],
            compiler_params=pltpu.CompilerParams(collective_id=1, has_side_effects=True, vmem_limit_bytes=32 * MB),
        )(tok, dy, g_own, *hops, ru, rv)
        du, dv, y, dx = pl.pallas_call(
            put_kernel,
            out_shape=[table, table, block, block],
            in_specs=[VMEM] * 4 + [SMEM, VMEM, HBM], out_specs=[HBM, HBM, VMEM, VMEM],
            scratch_shapes=[
                pltpu.VMEM((512, width), BF16), pltpu.VMEM((4096, width), BF16), pltpu.VMEM((4096, width), BF16),
                dma, dma((2,)),
            ],
            input_output_aliases={6: 0},
            compiler_params=pltpu.CompilerParams(vmem_limit_bytes=36 * MB),
        )(pu, pv, y, dx, vslot, meta, du)
        return y, dx, du, dv

    return jax.shard_map(device_step, mesh=mesh, in_specs=(tok_spec, tok_spec, row_spec, row_spec, tok_spec, tok_spec, tok_spec), out_specs=(tok_spec, tok_spec, row_spec, row_spec), check_vma=False)
```

```python
import functools

import jax
import jax.numpy as jnp
from jax import lax
from jax.experimental import pallas as pl
from jax.experimental.pallas import tpu as pltpu
from jax.sharding import PartitionSpec as P

MESH = pl.DeviceIdType.MESH
F32 = jnp.float32
BF16 = jnp.bfloat16
VMEM = pl.BlockSpec(memory_space=pltpu.VMEM)
ANY = pl.BlockSpec(memory_space=pl.ANY)
NT = (((1,), (1,)), ((), ()))
TN = (((0,), (0,)), ((), ()))
HBM = pl.BlockSpec(memory_space=pltpu.HBM)
SMEM = pl.BlockSpec(memory_space=pltpu.SMEM)
MB = 1024 * 1024
UP, DOWN, YY, CC = range(4)
EARLY = 2048
OTHERS = (2, 1, 3)
ALL3 = (0, 1, 2)
PAIR = (0, 1)


def gelu_pair(pre_act):
    cdf_val = 0.5 * (1.0 + lax.erf(pre_act * 0.7071067811865476))
    pdf_val = jnp.exp(-0.5 * pre_act * pre_act) * 0.3989422804014327
    return pre_act * cdf_val, cdf_val + pre_act * pdf_val


def split3(val):
    one = val.astype(BF16)
    rest = val - one.astype(F32)
    two = rest.astype(BF16)
    three = (rest - two.astype(F32)).astype(BF16)
    return one, two, three


def dot(a, b, dims=None):
    if dims is None:
        return jnp.dot(a, b, preferred_element_type=F32)
    return lax.dot_general(a, b, dims, preferred_element_type=F32)


def thirds(val):
    one, two, three = jnp.split(val, 3, axis=0)
    return one + two + three


def seg(i, n):
    return pl.ds(pl.multiple_of(i * n, n), n)


def iota(shape, axis):
    return lax.broadcasted_iota(jnp.int32, shape, axis)


def first_kernel(ids_ref, x_hbm, dy_hbm, pick_hbm, gate_hbm, ids_out, g_out, xd, dyd, xu, dyu, xy, dyy,
                 x_ref, dy_ref, pick_ref, gate_ref, lsem, ssem, rsem, hops, hopr):
    z = lax.axis_index("data")
    t = lax.axis_index("table")
    me = z * 4 + t
    bar = pltpu.get_barrier_semaphore()
    peers = [(lax.rem(z + dz, 4), lax.rem(t + dt, 4)) for dz in range(4) for dt in range(4)][1:]
    for pz, pt in peers:
        pl.semaphore_signal(bar, inc=1, device_id={"data": pz, "table": pt}, device_id_type=MESH)
    loads = [
        pltpu.make_async_copy(src, dst, lsem.at[i])
        for i, (src, dst) in enumerate(((pick_hbm, pick_ref), (gate_hbm, gate_ref), (x_hbm, x_ref), (dy_hbm, dy_ref)))
    ]
    for one in loads:
        one.start()
    loads[0].wait()
    loads[1].wait()

    sel, tok = pick_ref.shape
    quarter = sel // 4
    row = iota((2 * quarter, 2 * tok), 0)
    row = row + jnp.where(row >= quarter, quarter, 0)

    def add_gates(i, acc):
        pick8 = pick_ref[seg(i, 8), :]
        gate8 = gate_ref[seg(i, 8), :]
        pick8 = jnp.concatenate([pick8, pick8 - quarter], axis=1)
        gate8 = jnp.concatenate([gate8, gate8], axis=1)
        for j in range(8):
            acc = acc + jnp.where(row == pick8[j : j + 1, :], gate8[j : j + 1, :], 0.0)
        return acc

    g_out[...] = lax.fori_loop(0, sel // 8, add_gates, jnp.zeros((2 * quarter, 2 * tok), F32))
    loads[2].wait()
    loads[3].wait()
    pl.semaphore_wait(bar, 15)
    copies = []
    for i, (pz, pt) in enumerate(peers):
        copies.append(pltpu.make_async_remote_copy(
            src_ref=ids_ref, dst_ref=ids_out.at[me], send_sem=ssem.at[i], recv_sem=rsem.at[i],
            device_id={"data": pz, "table": pt}, device_id_type=MESH,
        ))
        copies[-1].start()

    def hop(k, lane):
        dst = ((xd, dyd), (xu, dyu), (xy, dyy))[lane][k]
        peer = ({"data": z + 1}, {"data": z - 1}, {"table": lax.rem(t + 2, 4)})[lane]
        return pltpu.make_async_remote_copy(
            src_ref=(x_ref, dy_ref)[k], dst_ref=dst, send_sem=hops.at[k, lane], recv_sem=hopr.at[k, lane],
            device_id=peer, device_id_type=MESH,
        )

    for k in PAIR:
        hop(k, 2).start()

        @pl.when(z < 3)
        def _():
            hop(k, 0).start()

        @pl.when(z > 0)
        def _():
            hop(k, 1).start()

    local = pltpu.make_async_copy(ids_ref, ids_out.at[me], ssem.at[15])
    local.start()
    local.wait()
    for one in copies:
        one.wait()
    for k in PAIR:
        hop(k, 2).wait()

        @pl.when(z < 3)
        def _():
            hop(k, 0).wait_send()
            hop(k, 1).wait_recv()

        @pl.when(z > 0)
        def _():
            hop(k, 1).wait_send()
            hop(k, 0).wait_recv()


def prep_kernel(u_hbm, v_hbm, ids_ref, du_hbm, dv_hbm, rows_u, rows_v, vslot, meta,
                zbuf, ugrp, vgrp, uacc, vacc, sslot, zsem, gsem, ssem):
    r = lax.axis_index("table")
    n_local = u_hbm.shape[0]
    n_ent = rows_u.shape[0]
    zrows = zbuf.shape[0]
    zbuf[...] = jnp.zeros_like(zbuf)

    ids = jnp.concatenate([ids_ref[e] for e in range(16)], axis=0).astype(F32)
    pick = ids[:, 0:32]
    for o in range(1, 4):
        pick = jnp.where(r == o, ids[:, o * 32 : o * 32 + 32], pick)
    pick = pick - (r * n_local).astype(F32)
    idrow = jnp.concatenate([pick[e : e + 1, :] for e in range(16)], axis=1)
    ii = iota((n_ent, n_ent), 0)
    jj = iota((n_ent, n_ent), 1)

    fills = [pltpu.make_async_copy(zbuf, du_hbm.at[pl.ds(i, zrows), :], zsem) for i in range(0, n_local, zrows)]
    fills += [pltpu.make_async_copy(zbuf, dv_hbm.at[pl.ds(i, zrows), :], zsem) for i in range(0, EARLY, zrows)]
    for one in fills:
        one.start()

    def lanes(cond, val):
        return jnp.sum(jnp.where(cond, val, 0.0), axis=1, keepdims=True)

    def subl(cond, val):
        return jnp.sum(jnp.where(cond, val, 0.0), axis=0, keepdims=True)

    idcol = lanes(ii == jj, jnp.broadcast_to(idrow, (n_ent, n_ent)))
    grow, gcol = jnp.floor(idrow * 0.125), jnp.floor(idcol * 0.125)
    same = gcol == grow
    lead_col = jnp.where(lanes(same & (jj < ii), 1.0) == 0.0, 1.0, 0.0)
    lead_row = jnp.where(subl(same & (ii < jj), 1.0) == 0.0, 1.0, 0.0)
    rank_col = lanes(jj < ii, jnp.broadcast_to(lead_row, (n_ent, n_ent)))
    rank_row = subl(ii < jj, jnp.broadcast_to(lead_col, (n_ent, n_ent)))
    hit_c = (rank_col.astype(jnp.int32) == jj) & (lead_col > 0.0)
    hit_r = (rank_row.astype(jnp.int32) == ii) & (lead_row > 0.0)
    icount = jnp.sum(lead_row, axis=1, keepdims=True).astype(jnp.int32)
    slot_row = subl(hit_c, jnp.broadcast_to(gcol, (n_ent, n_ent)))
    slot_col = lanes(hit_r, jnp.broadcast_to(grow, (n_ent, n_ent)))
    vslot[0:1, :] = slot_row.astype(jnp.int32)
    vslot[1:8, :] = jnp.broadcast_to(icount, (7, n_ent))
    slot_row = jnp.where(jj[0:1, :] < icount, slot_row, -1.0)
    slot_col = jnp.where(ii[:, 0:1] < icount, slot_col, -1.0)
    meta[0:1, :] = idrow
    meta[1:8, :] = jnp.broadcast_to(slot_row, (7, n_ent))

    to_smem = pltpu.make_async_copy(vslot, sslot, ssem)
    to_smem.start()
    to_smem.wait()
    n_blk = (sslot[1, 0] + 31) // 32

    def fetch(k, table, grp, s):
        g = seg(sslot[0, k], 8)
        return pltpu.make_async_copy(table.at[g, :], grp.at[seg(k, 8), :], gsem.at[s])

    def start_fetch(k, carry):
        fetch(k, u_hbm, ugrp, 0).start()
        fetch(k, v_hbm, vgrp, 1).start()
        return carry

    def wait_fetch(k, carry):
        fetch(k, u_hbm, ugrp, 0).wait()
        fetch(k, v_hbm, vgrp, 1).wait()
        return carry

    lax.fori_loop(0, n_blk * 32, start_fetch, 0)
    lax.fori_loop(0, n_blk * 32, wait_fetch, 0)

    uacc[...] = jnp.zeros_like(uacc)
    vacc[...] = jnp.zeros_like(vacc)
    kk = iota((n_ent, 256), 0)
    qk = iota((n_ent, 256), 1) >> 3
    q7 = (iota((1, 256), 1) & 7).astype(F32)

    def take_rows(b, carry):
        rowid = 8.0 * subl(kk == qk + b * 32, jnp.broadcast_to(slot_col, (n_ent, 256))) + q7
        pickm = jnp.where(idcol == rowid, 1.0, 0.0).astype(BF16)
        base = seg(b, 256)
        uacc[...] += dot(pickm, ugrp[base, :])
        vacc[...] += dot(pickm, vgrp[base, :])
        return carry

    lax.fori_loop(0, n_blk, take_rows, 0)
    rows_u[...] = uacc[...].astype(BF16)
    rows_v[...] = vacc[...].astype(BF16)
    for one in fills:
        one.wait()


def main_kernel(x_ref, dy_ref, g_ref, xd, dyd, xu, dyu, xy, dyy, ru, rv, pu, pv, y_out, dx_out,
                tx, ty, gx, ubuf, vbuf, ssem, rsem, rows_s, rows_r):
    z = lax.axis_index("data")
    t = lax.axis_index("table")
    y, c = t // 2, lax.rem(t, 2)
    t_y = (1 - y) * 2 + c
    t_c = y * 2 + (1 - c)
    t_yc = (1 - y) * 2 + (1 - c)
    y_peer, c_peer = {"table": t_y}, {"table": t_c}
    up, down = {"data": z + 1}, {"data": z - 1}
    peers = {UP: up, DOWN: down, YY: y_peer, CC: c_peer}
    tok = x_ref.shape[0]
    low_at = {d: z - d >= 0 for d in OTHERS}
    high_at = {d: z + d <= 3 for d in OTHERS}
    can_up, can_down = high_at[1], low_at[1]
    middle = can_up & can_down
    ends = (z == 0) | (z == 3)

    bar = pltpu.get_barrier_semaphore()
    for peer in (t_y, t_c, t_yc):
        pl.semaphore_signal(bar, inc=1, device_id={"table": peer}, device_id_type=MESH)

    @pl.when(can_up)
    def _():
        pl.semaphore_signal(bar, inc=1, device_id=up, device_id_type=MESH)

    @pl.when(can_down)
    def _():
        pl.semaphore_signal(bar, inc=1, device_id=down, device_id_type=MESH)

    pl.semaphore_wait(bar, 3 + can_up.astype(jnp.int32) + can_down.astype(jnp.int32))

    outs = (gx, tx, ty)
    TOKS = (1, 2)
    sent = []

    def place(k, slot):
        if k == 0:
            return gx.at[slot]
        return outs[k].at[seg(slot, tok), :]

    def copy(k, slot, lane, src=None):
        ref = place(k, slot)
        return pltpu.make_async_remote_copy(
            src_ref=ref if src is None else src, dst_ref=ref,
            send_sem=ssem.at[k, lane, slot], recv_sem=rsem.at[k, slot],
            device_id=peers[lane], device_id_type=MESH,
        )

    def when(cond, run):
        if cond is None:
            run()
        else:
            @pl.when(cond)
            def _():
                run()

    def start(cond, k, slot, lane, src=None):
        sent.append((cond, k, slot, lane))
        when(cond, lambda: copy(k, slot, lane, src).start())

    def arrive(cond, k, slot):
        when(cond, lambda: copy(k, slot, CC).wait_recv())

    def zs(d):
        return (z + d) * 4 + t

    def ys(d):
        return (z + d) * 4 + t_y

    def send_row(k, s):
        to = lax.rem(t + s, 4)
        return pltpu.make_async_remote_copy(
            src_ref=(ru, rv)[k].at[seg(z * 4 + to, 32), :],
            dst_ref=(ubuf, vbuf)[k].at[seg(t, 32), :],
            send_sem=rows_s.at[k, s], recv_sem=rows_r.at[k, s],
            device_id={"table": to}, device_id_type=MESH,
        )

    own = (None, x_ref, dy_ref)
    low = (None, xd, dyd)
    high = (None, xu, dyu)
    across = (None, xy, dyy)
    me = zs(0)
    my_half = g_ref.at[seg(y, 32), :]
    other_half = g_ref.at[seg(1 - y, 32), :]

    start(can_up, 0, me, UP, my_half)
    start(can_down, 0, me, DOWN, my_half)
    start(None, 0, me, YY, other_half)
    start(None, 0, me, CC, my_half)
    for k in TOKS:
        start(middle, k, zs(-1), UP, low[k])
        start(middle, k, zs(1), DOWN, high[k])
    for k in PAIR:
        for s in OTHERS:
            send_row(k, s).start()
    for k in TOKS:
        start(None, k, me, CC, own[k])
        start(None, k, ys(0), CC, across[k])
        start(can_down, k, zs(-1), CC, low[k])
        start(can_up, k, zs(1), CC, high[k])

    def keep(cond, k, slot, src):
        def run():
            outs[k][seg(slot, tok), :] = src[...]

        when(cond, run)

    gx[me] = g_ref[seg(y, 32), :]
    for k in TOKS:
        keep(None, k, me, own[k])
        keep(None, k, ys(0), across[k])
        keep(can_down, k, zs(-1), low[k])
        keep(can_up, k, zs(1), high[k])
    mine = seg(t, 32)
    ubuf[mine, :] = ru[seg(z * 4 + t, 32), :]
    vbuf[mine, :] = rv[seg(z * 4 + t, 32), :]

    def gates_on(slot_of, d, from_low=None, from_high=None):
        from_low = low_at[d] if from_low is None else from_low
        from_high = high_at[d] if from_high is None else from_high
        arrive(from_low, 0, slot_of(-d))
        start(from_low & can_up, 0, slot_of(-d), UP)
        start(from_low, 0, slot_of(-d), CC)
        arrive(from_high, 0, slot_of(d))
        start(from_high & can_down, 0, slot_of(d), DOWN)
        start(from_high, 0, slot_of(d), CC)

    def tokens_on(d):
        for k in TOKS:
            arrive(low_at[d], k, zs(-d))
            start(low_at[d] & can_up, k, zs(-d), UP)
            start(low_at[d], k, zs(-d), YY)
            arrive(high_at[d], k, zs(d))
            start(high_at[d] & can_down, k, zs(d), DOWN)
            start(high_at[d], k, zs(d), YY)
            start(low_at[d], k, zs(-d), CC)
            start(high_at[d], k, zs(d), CC)

    def crossed(cond, d):
        for k in TOKS:
            arrive(cond, k, ys(d))
            start(cond, k, ys(d), CC)

    diag = (iota((128, 256), 0) >> 5) == (iota((128, 256), 1) >> 6)

    def products(d):
        for tt in (t_c, t_yc):
            for k in ALL3:
                arrive(None, k, d * 4 + tt)
        tsl = seg(d, 256)
        esl = seg(d, 128)
        x4, dy4 = tx[tsl, :], ty[tsl, :]
        u4, v4 = ru[esl, :], rv[esl, :]
        gates = []
        for e in range(4):
            part = gx[d * 4 + e]
            part = jnp.where(c == 1, part[:, 64:128], part[:, 0:64])
            gates.append(jnp.concatenate([part] * 4, axis=1))
        g4 = jnp.concatenate(gates, axis=0)
        act, slope = gelu_pair(dot(u4, x4, NT))
        b4 = dot(v4, dy4, NT)
        w4 = jnp.where(diag, g4 * act, 0.0)
        c4 = jnp.where(diag, g4 * slope * b4, 0.0)
        for coef, val, out in ((c4, x4, pu), (w4, dy4, pv)):
            full = dot(jnp.concatenate(split3(coef), axis=0), val)
            full = thirds(full)
            for k, term in enumerate(split3(full)):
                out[k, esl, :] = term

    def cross_on(go_up, go_down):
        for k in ALL3:
            start(go_up, k, ys(0), UP, across[k])
            start(go_down, k, ys(0), DOWN, across[k])

    gates_on(zs, 1)
    arrive(None, 0, ys(0))
    cross_on(z < 2, z > 1)
    start(None, 0, ys(0), CC)
    products(z)
    tokens_on(2)
    gates_on(zs, 2)
    gates_on(ys, 1, middle, middle)
    cross_on(z == 2, z == 1)

    gates = jnp.concatenate([g_ref[0:32, 0:64], g_ref[0:32, 64:128], g_ref[32:64, 0:64], g_ref[32:64, 64:128]], axis=0)
    for s in OTHERS:
        send_row(0, s).wait_recv()
        send_row(1, s).wait_recv()
    act, slope = gelu_pair(dot(ubuf[...], x_ref[...], NT))
    b_val = dot(vbuf[...], dy_ref[...], NT)
    w_val = jnp.transpose(gates * act)
    c_val = jnp.transpose(gates * slope * b_val)
    for coef, rows, out in ((w_val, vbuf, y_out), (c_val, ubuf, dx_out)):
        full = dot(jnp.concatenate(split3(coef), axis=0), rows[...])
        out[...] = (thirds(full)).astype(BF16)

    tokens_on(3)
    gates_on(zs, 3)
    crossed(middle, -1)
    crossed(middle, 1)
    gates_on(ys, 2)
    when(middle, lambda: products(z - 1))
    when(middle, lambda: products(z + 1))
    crossed(low_at[2], -2)
    crossed(high_at[2], 2)
    products(lax.rem(z + 2, 4))
    gates_on(ys, 1, z == 3, z == 0)
    crossed(z == 3, -1)
    crossed(z == 0, 1)
    crossed(low_at[3], -3)
    crossed(high_at[3], 3)
    gates_on(ys, 3)
    when(ends, lambda: products(1 + z // 3))
    when(ends, lambda: products(3 - z))

    for k in PAIR:
        for s in OTHERS:
            send_row(k, s).wait_send()
    for cond, k, slot, lane in sent:
        when(cond, lambda k=k, slot=slot, lane=lane: copy(k, slot, lane).wait_send())


def put_kernel(pu, pv, y_ref, dx_ref, sslot, meta, du_in, dv_in, du_hbm, dv_hbm, y_out, dx_out,
               zbuf, ures, vres, zsem, psem):
    n_ent = pu.shape[1]
    zrows = zbuf.shape[0]
    zbuf[...] = jnp.zeros_like(zbuf)
    y_out[...] = y_ref[...]
    dx_out[...] = dx_ref[...]
    n_slot = sslot[1, 0]
    n_blk = (n_slot + 31) // 32
    idrow, slot_row = meta[0:1, :], meta[1:2, :]
    fills = [pltpu.make_async_copy(zbuf, dv_hbm.at[pl.ds(i, zrows), :], zsem) for i in range(EARLY, dv_hbm.shape[0], zrows)]
    for one in fills:
        one.start()
    kq = iota((256, n_ent), 1)
    qq = iota((256, n_ent), 0) >> 3
    q7 = (iota((256, 1), 0) & 7).astype(F32)

    def patch(k, table, res, s):
        g = seg(sslot[0, k], 8)
        return pltpu.make_async_copy(res.at[seg(k, 8), :], table.at[g, :], psem.at[s])

    def over_slots(lo, hi, run):
        def body(k, carry):
            run(k)
            return carry

        lax.fori_loop(lo, hi, body, 0)

    def put_rows(b, carry):
        rowid = 8.0 * jnp.sum(jnp.where(kq == qq + b * 32, slot_row, 0.0), axis=1, keepdims=True) + q7
        spread = jnp.where(rowid == idrow, 1.0, 0.0).astype(BF16)
        base = seg(b, 256)
        ures[base, :] = (dot(spread, pu[0]) + dot(spread, pu[1]) + dot(spread, pu[2])).astype(BF16)
        vres[base, :] = (dot(spread, pv[0]) + dot(spread, pv[1]) + dot(spread, pv[2])).astype(BF16)
        over_slots(b * 32, jnp.minimum(b * 32 + 32, n_slot), lambda k: patch(k, du_hbm, ures, 0).start())
        return carry

    lax.fori_loop(0, n_blk, put_rows, 0)
    for one in fills:
        one.wait()
    over_slots(0, n_slot, lambda k: patch(k, dv_hbm, vres, 1).start())
    over_slots(0, n_slot, lambda k: patch(k, du_hbm, ures, 0).wait())
    over_slots(0, n_slot, lambda k: patch(k, dv_hbm, vres, 1).wait())


def in_hbm(*vals):
    return [pltpu.with_memory_space_constraint(val, pltpu.HBM) for val in vals]


def solution(mesh):
    tok_spec = P(('replica', 'data', 'table'))
    row_spec = P(('replica', 'table'))

    def device_step(tok, dy, u, v, wanted, pick, gate):
        n_tok, width = tok.shape
        n_local = u.shape[0]
        sel = pick.shape[1] * pick.shape[2]
        shape = jax.ShapeDtypeStruct
        dma = pltpu.SemaphoreType.DMA
        rows = shape((512, width), BF16)
        block = shape((n_tok, width), BF16)
        table = shape((n_local, width), BF16)
        pick_t = jnp.transpose(pick, (1, 2, 0)).reshape(sel, n_tok)
        gate_t = jnp.transpose(gate, (1, 2, 0)).reshape(sel, n_tok)

        ids, g_own, *hops = pl.pallas_call(
            first_kernel,
            out_shape=[shape((16, 1, 128), jnp.int32), shape((64, 128), F32)] + [block] * 6,
            in_specs=[HBM] * 5, out_specs=[VMEM] * 8,
            scratch_shapes=[
                pltpu.VMEM((n_tok, width), BF16), pltpu.VMEM((n_tok, width), BF16),
                pltpu.VMEM((sel, n_tok), jnp.int32), pltpu.VMEM((sel, n_tok), F32),
                dma((4,)), dma((16,)), dma((15,)), dma((2, 3)), dma((2, 3)),
            ],
            compiler_params=pltpu.CompilerParams(collective_id=0, has_side_effects=True, vmem_limit_bytes=4 * MB),
        )(*in_hbm(wanted, tok, dy, pick_t, gate_t))
        du, dv, ru, rv, vslot, meta = pl.pallas_call(
            prep_kernel,
            out_shape=[table, table, rows, rows, shape((8, 512), jnp.int32), shape((8, 512), F32)],
            in_specs=[HBM] * 2 + [VMEM], out_specs=[HBM] * 2 + [VMEM] * 4,
            scratch_shapes=[
                pltpu.VMEM((512, width), BF16), pltpu.VMEM((4096, width), BF16), pltpu.VMEM((4096, width), BF16),
                pltpu.VMEM((512, width), F32), pltpu.VMEM((512, width), F32),
                pltpu.SMEM((8, 512), jnp.int32), dma, dma((2,)), dma,
            ],
            compiler_params=pltpu.CompilerParams(vmem_limit_bytes=36 * MB),
        )(u, v, ids)
        pu, pv, y, dx = pl.pallas_call(
            main_kernel,
            out_shape=[shape((3, 512, width), BF16)] * 2 + [block] * 2,
            in_specs=[VMEM] * 11, out_specs=[VMEM] * 4,
            scratch_shapes=[
                pltpu.VMEM((16 * n_tok, width), BF16), pltpu.VMEM((16 * n_tok, width), BF16),
                pltpu.VMEM((16, 32, 128), F32), pltpu.VMEM((128, width), BF16), pltpu.VMEM((128, width), BF16),
                dma((3, 4, 16)), dma((3, 16)), *[dma((2, 4))] * 2,
            ],
            compiler_params=pltpu.CompilerParams(collective_id=1, has_side_effects=True, vmem_limit_bytes=32 * MB),
        )(tok, dy, g_own, *hops, ru, rv)
        du, dv, y, dx = pl.pallas_call(
            put_kernel,
            out_shape=[table, table, block, block],
            in_specs=[VMEM] * 4 + [SMEM, VMEM, HBM, HBM], out_specs=[HBM, HBM, VMEM, VMEM],
            scratch_shapes=[
                pltpu.VMEM((512, width), BF16), pltpu.VMEM((4096, width), BF16), pltpu.VMEM((4096, width), BF16),
                dma, dma((2,)),
            ],
            input_output_aliases={6: 0, 7: 1},
            compiler_params=pltpu.CompilerParams(vmem_limit_bytes=36 * MB),
        )(pu, pv, y, dx, vslot, meta, du, dv)
        return y, dx, du, dv

    return jax.shard_map(device_step, mesh=mesh, in_specs=(tok_spec, tok_spec, row_spec, row_spec, tok_spec, tok_spec, tok_spec), out_specs=(tok_spec, tok_spec, row_spec, row_spec), check_vma=False)
```
